256 devices in a mesh: gx: 8 (over y, core), gy: 32 (over x, z).
Axes of the slice: x: 4, y: 4, z: 8, core: 2. Of those that a mesh axis runs over, the one named last changes fastest.
Arguments:
- previous: float32 [2, 7, 1024, 4096], P(None, None, 'gx', 'gy'), may hold values from -6 to 6
- dissipated: float32 [2, 4, 1024, 4096], P(None, None, 'gx', 'gy'), may hold values from 0.05 to 3
- material: int32 [4, 1024, 4096], P(None, 'gx', 'gy'), may hold values from 0 to 3
- coolant: int32 [3, 1024, 4096], P(None, 'gx', 'gy'), may hold values from 0 to 3
Outputs:
- temperature: float32 [2, 7, 1024, 4096], P(None, None, 'gx', 'gy')
The draws below stay inside these ranges and needn't reach their ends.
All inputs are finite; a program needn't handle non-finite values.
Results may differ from the reference program's by a relative error of at most 0.00011.
Values sent between devices are 32-bit elements; how exact they have to be, the bound alone decides.
No kernel may reach another device: no remote copies, remote signals or barrier semaphores. Data moves between devices by JAX's collectives and lax.ppermute only.
A program may use at most 64 MiB of HBM per device.

```python
import math
import jax
import jax.numpy as jnp
from jax import lax

TIERS = 4
CHANNELS = 3
LAYERS = 7
SCEN = 2
ITERS = 3
NX = 1024
NY = 4096


def set_ends(entries, stream_key, low, largest):
    longest = entries.shape.index(max(entries.shape))
    spots = []
    for shift in (0, 1):
        where = [jax.random.randint(jax.random.fold_in(stream_key, axis), (), 0, length) for axis, length in enumerate(entries.shape)]
        where[longest] = (where[longest] + shift) % entries.shape[longest]
        spots.append(tuple(where))
    return entries.at[spots[0]].set(low).at[spots[1]].set(largest)


def block_scale(key, dims, split, low, largest):
    def one(position, shards_of):
        steps = jax.random.uniform(jax.random.fold_in(jax.random.fold_in(key, 6), position), (shards_of,), jnp.float32, low / len(split), largest / len(split))
        return jnp.repeat(jnp.exp(steps), dims[position] // shards_of).reshape((-1,) + (1,) * (len(dims) - position - 1))

    level = one(*split[0])
    for cut in split[1:]:
        level = level * one(*cut)
    return level


def bell_draw(key, shape, deviation, bound, cuts=(), dtype=jnp.bfloat16):
    result = jax.random.normal(key, shape, jnp.float32) * deviation
    if len(cuts) > 0:
        result = block_scale(key, shape, cuts, -0.22, 0.18) * result
    return jnp.clip(result, min=-bound, max=bound).astype(dtype)


def setup_inputs(seed: int = 0) -> dict:
    streams_of = jax.random.split(jax.random.key(seed), 5)
    previous = bell_draw(streams_of[0], (SCEN, LAYERS, NX, NY), 1.0, 6.0, ((2, 8), (3, 32)), jnp.float32)
    dissipated = jnp.clip(jnp.exp(math.log(3.0) - 4.0943445 * jax.random.uniform(streams_of[1], (SCEN, TIERS, NX, NY), jnp.float32) ** block_scale(streams_of[1], (SCEN, TIERS, NX, NY), ((2, 8), (3, 32)), -0.2, 0.2)), 0.05, 3.0)
    material = set_ends(jax.random.randint(streams_of[2], (TIERS, NX, NY), 0, 4), jax.random.fold_in(streams_of[2], 1), 0, 3).astype(jnp.int32)
    coolant = set_ends(jax.random.randint(streams_of[3], (CHANNELS, NX, NY), 0, 4), jax.random.fold_in(streams_of[3], 1), 0, 3).astype(jnp.int32)
    return dict(previous=previous, dissipated=dissipated, material=material, coolant=coolant)


TIER_K = (1.0, 0.3, 0.12, 2.5)
CHANNEL_K = (1.0, 0.3, 0.25, 0.2)
CHANNEL_SINK = (0.0, 0.15, 0.45, 1.2)
TIER_HEAT = 0.05
CHANNEL_HEAT = 0.2
VERTICAL = 4.0

def lookup(codes, table):
    total = jnp.zeros(codes.shape, jnp.float32)
    for index, value in enumerate(table):
        total = total + jnp.where(codes == index, jnp.float32(value), jnp.float32(0.0))
    return total

def mix(tiers, channels):
    rows = []
    for layer in range(2 * tiers.shape[0] - 1):
        rows.append(tiers[layer // 2] if layer % 2 == 0 else channels[layer // 2])
    return jnp.stack(rows)

def capacity_column(layers):
    return jnp.array([TIER_HEAT if layer % 2 == 0 else CHANNEL_HEAT for layer in range(layers)], jnp.float32)

def couplings(padded_k):
    centre = padded_k[:, 1:-1, 1:-1]
    g_north = jnp.sqrt(centre * padded_k[:, :-2, 1:-1])
    g_south = jnp.sqrt(centre * padded_k[:, 2:, 1:-1])
    g_west = jnp.sqrt(centre * padded_k[:, 1:-1, :-2])
    g_east = jnp.sqrt(centre * padded_k[:, 1:-1, 2:])
    g_vertical = VERTICAL * jnp.sqrt(centre[:-1] * centre[1:])
    return (g_north, g_south, g_west, g_east, g_vertical)

def operate(padded_v, padded_k, sink, capacity):
    g_north, g_south, g_west, g_east, g_vertical = couplings(padded_k)
    centre = padded_v[:, 1:-1, 1:-1]
    lateral = g_north * (centre - padded_v[:, :-2, 1:-1]) + g_south * (centre - padded_v[:, 2:, 1:-1])
    lateral = lateral + g_west * (centre - padded_v[:, 1:-1, :-2]) + g_east * (centre - padded_v[:, 1:-1, 2:])
    flux = g_vertical * (centre[:-1] - centre[1:])
    zero_row = jnp.zeros_like(centre[:1])
    vertical = jnp.concatenate([flux, zero_row], 0) - jnp.concatenate([zero_row, flux], 0)
    return (capacity + sink) * centre + lateral + vertical

def diagonal_terms(padded_k, sink, capacity):
    g_north, g_south, g_west, g_east, g_vertical = couplings(padded_k)
    zero_row = jnp.zeros_like(g_vertical[:1])
    vertical = jnp.concatenate([g_vertical, zero_row], 0) + jnp.concatenate([zero_row, g_vertical], 0)
    return capacity + sink + g_north + g_south + g_west + g_east + vertical

def padded(field):
    return jnp.pad(field, ((0, 0), (1, 1), (1, 1)))

def reference(previous, dissipated, material, coolant):
    tier_k = lookup(material, TIER_K)
    kappa = mix(tier_k, lookup(coolant, CHANNEL_K))
    sink = mix(jnp.zeros_like(tier_k), lookup(coolant, CHANNEL_SINK))
    capacity = capacity_column(kappa.shape[0])[:, None, None]
    padded_k = padded(kappa)
    diagonal = diagonal_terms(padded_k, sink, capacity)

    def solve_one(pair):
        start, heat = pair
        source = capacity * start + mix(heat, jnp.zeros_like(heat[:-1]))
        residual = source - operate(padded(start), padded_k, sink, capacity)
        solution = start
        scaled = residual / diagonal
        norm_now = jnp.sum(residual * scaled)
        direction = scaled
        for iteration in range(ITERS):
            image = operate(padded(direction), padded_k, sink, capacity)
            step_size = norm_now / jnp.sum(direction * image)
            solution = solution + step_size * direction
            residual = residual - step_size * image
            if iteration + 1 < ITERS:
                scaled = residual / diagonal
                norm_next = jnp.sum(residual * scaled)
                direction = scaled + norm_next / norm_now * direction
                norm_now = norm_next
        return solution
    return lax.map(solve_one, (previous, dissipated))
```

```python
import functools

import jax
import jax.numpy as jnp
from jax import lax
from jax.experimental import pallas as pl
from jax.experimental.pallas import tpu as pltpu
from jax.sharding import PartitionSpec as P

TIER_K = (1.0, 0.3, 0.12, 2.5)
CHANNEL_K = (1.0, 0.3, 0.25, 0.2)
CHANNEL_SINK = (0.0, 0.15, 0.45, 1.2)
TIER_HEAT = 0.05
CHANNEL_HEAT = 0.2
VERTICAL = 4.0

SCEN, TIERS, LAYERS = 2, 4, 7
TILE = 128
HALO = 4
FIELDS = SCEN * LAYERS + SCEN * TIERS + LAYERS
DISS = SCEN * LAYERS
CODE = DISS + SCEN * TIERS
TOP = 16
ROWS = TOP + TILE + 16
F32 = jnp.float32


def tables(layer):
    if layer % 2 == 0:
        kappa, sink, heat = TIER_K, (0.0,) * 4, TIER_HEAT
    else:
        kappa, sink, heat = CHANNEL_K, CHANNEL_SINK, CHANNEL_HEAT
    root = [k**0.5 for k in kappa]
    return (
        (0.0, *root),
        (0.0, *[1.0 / r for r in root]),
        (1.0, *[(heat + s) / r for s, r in zip(sink, root)]),
        (0.0, *[s / r for s, r in zip(sink, root)]),
    )


def pick(code, table):
    out = jnp.full(code.shape, table[0], F32)
    for index in range(1, 5):
        out = jnp.where(code == float(index), F32(table[index]), out)
    return out


def code_of(material, coolant, layer, rows):
    block = material[layer // 2, rows] if layer % 2 == 0 else coolant[layer // 2, rows]
    return block.astype(F32) + 1.0


def field_rows(previous, dissipated, material, coolant, field, rows):
    if field < DISS:
        return previous[field // LAYERS, field % LAYERS, rows]
    if field < CODE:
        return dissipated[(field - DISS) // TIERS, (field - DISS) % TIERS, rows]
    return code_of(material, coolant, field - CODE, rows)


def pack_rows(pt, pb, dt, db, mt, mb, ct, cb, a_out, b_out):
    lower = lax.axis_index("gx") % 2 == 0
    for field in range(FIELDS):
        top = field_rows(pt, dt, mt, ct, field, slice(0, HALO))
        bottom = field_rows(pb, db, mb, cb, field, slice(8 - HALO, 8))
        rows = slice(HALO * field, HALO * (field + 1))
        a_out[rows, :] = jnp.where(lower, bottom, top)
        b_out[rows, :] = jnp.where(lower, top, bottom)


def pack_columns(prev, diss, mat, cool, a_in, b_in, halo_out, a_out, b_out):
    lower = lax.axis_index("gx") % 2 == 0
    west = lax.axis_index("gy") % 2 == 0
    for field in range(FIELDS):
        rows = slice(HALO * field, HALO * (field + 1))
        halo_out[field, :HALO, :] = jnp.where(lower, b_in[rows, :], a_in[rows, :])
        halo_out[field, HALO:, :] = jnp.where(lower, a_in[rows, :], b_in[rows, :])
    lane = lax.broadcasted_iota(jnp.int32, (8, TILE), 1)

    def pack(get, rows):
        low = jnp.zeros((8, TILE), F32)
        high = jnp.zeros((8, TILE), F32)
        for field in range(FIELDS):
            x = get(field)
            at = HALO * field
            mine = (lane >= at) & (lane < at + HALO)
            low = jnp.where(mine, pltpu.roll(x, at, 1) if at else x, low)
            high = jnp.where(mine, pltpu.roll(x, at + HALO, 1), high)
        a_out[rows, :] = jnp.where(west, high, low)
        b_out[rows, :] = jnp.where(west, low, high)

    @pl.loop(0, TILE // 8)
    def _(k):
        rows = pl.ds(pl.multiple_of(8 * k, 8), 8)
        pack(lambda field: field_rows(prev, diss, mat, cool, field, rows), rows)

    pack(lambda field: halo_out[field], slice(TILE, TILE + 8))


def solve(prev, diss, mat, cool, halo, a_in, b_in, w0_out, w1_out, w2_out, m_out,
          sa, sb, ypa, ypb, xb, qa, qb, y0a, y0b, y1a, y1b, y2a, y2b):
    west = lax.axis_index("gy") % 2 == 0
    lane = lax.broadcasted_iota(jnp.int32, (8, TILE), 1)
    first, last = lane == 0, lane == TILE - 1
    zero = jnp.zeros((8, TILE), F32)

    def start(get, get_code, message_rows, stores):
        a, b = a_in[message_rows, :], b_in[message_rows, :]
        east = jnp.where(west, a, b)
        wst = jnp.where(west, b, a)

        def strip(field):
            at = HALO * field
            x = jnp.where(lane < HALO, pltpu.roll(east, (TILE - at) % TILE, 1) if at else east, zero)
            return jnp.where(lane >= TILE - HALO, pltpu.roll(wst, (2 * TILE - HALO - at) % TILE, 1), x)

        def put(ref, index, value):
            for rows, shift in stores:
                ref[index, rows, :] = pltpu.roll(value, shift, 0) if shift else value

        for layer in range(LAYERS):
            root = tables(layer)[0]
            s = pick(get_code(layer), root)
            put(sa, layer, s)
            c = strip(CODE + layer)
            put(xb, CODE + layer, c)
            s2 = pick(c, root)
            put(sb, layer, s2)
            for scen in range(SCEN):
                f = scen * LAYERS + layer
                put(ypa, f, s * get(f))
                x = strip(f)
                put(xb, f, x)
                put(ypb, f, s2 * x)
                if layer % 2 == 0:
                    d = DISS + scen * TIERS + layer // 2
                    put(xb, d, strip(d))

    @pl.loop(0, TILE // 8)
    def _(k):
        rows = pl.ds(pl.multiple_of(8 * k, 8), 8)
        start(
            lambda f: field_rows(prev, diss, mat, cool, f, rows),
            lambda layer: code_of(mat, cool, layer, rows),
            rows,
            ((pl.ds(pl.multiple_of(8 * k + TOP, 8), 8), 0),),
        )

    start(
        lambda f: halo[f],
        lambda layer: halo[CODE + layer],
        slice(TILE, TILE + 8),
        ((slice(TOP - 8, TOP), 4), (slice(TOP + TILE, TOP + TILE + 8), 4)),
    )

    def around(xa, xb_, base, r, both):
        here = pl.ds(r, 8)
        a = [xa[base + layer, here, :] for layer in range(LAYERS)]
        b = [xb_[base + layer, here, :] for layer in range(LAYERS)]
        out_a, out_b = [], []
        for layer in range(LAYERS):
            down_a, down_b = pltpu.roll(a[layer], 1, 1), pltpu.roll(b[layer], 1, 1)
            up_a, up_b = pltpu.roll(a[layer], TILE - 1, 1), pltpu.roll(b[layer], TILE - 1, 1)

            def total(x, x_ref, to_west, to_east):
                f = base + layer
                t = (x_ref[f, pl.ds(r - 1, 8), :] + x_ref[f, pl.ds(r + 1, 8), :]) + (to_west + to_east)
                if layer == 0:
                    return t + VERTICAL * x[1]
                if layer == LAYERS - 1:
                    return t + VERTICAL * x[layer - 1]
                return t + VERTICAL * (x[layer - 1] + x[layer + 1])

            out_a.append(total(a, xa, jnp.where(first, down_b, down_a), jnp.where(last, up_b, up_a)))
            if both:
                out_b.append(total(b, xb_, jnp.where(first, down_a, down_b), jnp.where(last, up_a, up_b)))
        return a, b, out_a, out_b

    def tree(terms):
        while len(terms) > 1:
            terms = [sum(terms[i : i + 2][1:], terms[i]) for i in range(0, len(terms), 2)]
        return terms[0]

    def first_step(r, main, get, get_code):
        here = pl.ds(r, 8)
        _, _, ssa, ssb = around(sa, sb, 0, r, True)
        q_a, q_b = [], []
        for layer in range(LAYERS):
            _, _, over, _ = tables(layer)
            s, s2 = sa[layer, here, :], sb[layer, here, :]
            q_a.append(s / (pick(get_code(layer), over) + ssa[layer]))
            q_b.append(s2 / (pick(xb[CODE + layer, here, :], over) + ssb[layer]))
            qa[layer, here, :] = q_a[-1]
            qb[layer, here, :] = q_b[-1]
        sums = []
        for scen in range(SCEN):
            base = scen * LAYERS
            _, _, ta, tb = around(ypa, ypb, base, r, True)
            products = []
            for layer in range(LAYERS):
                _, inverse, _, loss = tables(layer)
                f = base + layer
                d = DISS + scen * TIERS + layer // 2
                code, code2 = get_code(layer), xb[CODE + layer, here, :]
                t = ta[layer] - (pick(code, loss) + ssa[layer]) * get(f)
                t2 = tb[layer] - (pick(code2, loss) + ssb[layer]) * xb[f, here, :]
                if layer % 2 == 0:
                    t = t + get(d) * pick(code, inverse)
                    t2 = t2 + xb[d, here, :] * pick(code2, inverse)
                y = q_a[layer] * t
                y0a[f, here, :] = y
                y0b[f, here, :] = q_b[layer] * t2
                products.append(y * t)
            sums.append(tree(products))
        return tuple(sums) if main else None

    def main_first(k, acc):
        rows = pl.ds(pl.multiple_of(8 * k, 8), 8)
        sums = first_step(
            pl.multiple_of(8 * k + TOP, 8),
            True,
            lambda f: field_rows(prev, diss, mat, cool, f, rows),
            lambda layer: code_of(mat, cool, layer, rows),
        )
        return tuple(a + s for a, s in zip(acc, sums))

    none = (zero,) * SCEN
    m0 = lax.fori_loop(0, TILE // 8, main_first, none)
    for r in (TOP - 8, TOP + TILE):
        first_step(r, False, lambda f: pltpu.roll(halo[f], 4, 0), lambda layer: pltpu.roll(halo[CODE + layer], 4, 0))

    def step(xa, xb_, na, nb, r):
        here = pl.ds(r, 8)
        odd, even = [], []
        for scen in range(SCEN):
            base = scen * LAYERS
            a, _, ta, tb = around(xa, xb_, base, r, True)
            p, p2 = [], []
            for layer in range(LAYERS):
                f = base + layer
                y = qa[layer, here, :] * ta[layer]
                na[f, here, :] = y
                nb[f, here, :] = qb[layer, here, :] * tb[layer]
                p.append(a[layer] * ta[layer])
                p2.append(y * ta[layer])
            odd.append(tree(p))
            even.append(tree(p2))
        return (*odd, *even)

    def sweep(xa, xb_, na, nb):
        def body(k, acc):
            return tuple(a + s for a, s in zip(acc, step(xa, xb_, na, nb, pl.multiple_of(8 * k + TOP, 8))))

        acc = lax.fori_loop(0, TILE // 8, body, none + none)
        for r in (TOP - 8, TOP + TILE):
            step(xa, xb_, na, nb, r)
        return acc[:SCEN], acc[SCEN:]

    m1, m2 = sweep(y0a, y0b, y1a, y1b)
    m3, m4 = sweep(y1a, y1b, y2a, y2b)

    def final(k, acc):
        rows = pl.ds(pl.multiple_of(8 * k, 8), 8)
        r = pl.multiple_of(8 * k + TOP, 8)
        here = pl.ds(r, 8)
        scale = [pick(code_of(mat, cool, layer, rows), tables(layer)[1]) for layer in range(LAYERS)]
        sums = []
        for scen in range(SCEN):
            base = scen * LAYERS
            a, _, ta, _ = around(y2a, y2b, base, r, False)
            sums.append(tree([a[layer] * ta[layer] for layer in range(LAYERS)]))
            for layer in range(LAYERS):
                f = base + layer
                w2_out[f, rows, :] = scale[layer] * a[layer]
                w1_out[f, rows, :] = scale[layer] * y1a[f, here, :]
                w0_out[f, rows, :] = scale[layer] * y0a[f, here, :]
        return tuple(x + s for x, s in zip(acc, sums))

    m5 = lax.fori_loop(0, TILE // 8, final, none)
    line = lax.broadcasted_iota(jnp.int32, (1, TILE), 1)
    out = jnp.zeros((1, TILE), F32)
    for index, moment in enumerate((m0, m1, m2, m3, m4, m5)):
        for scen in range(SCEN):
            value = jnp.sum(jnp.sum(moment[scen], axis=0, keepdims=True), axis=1, keepdims=True)
            out = jnp.where(line == SCEN * index + scen, value, out)
    m_out[...] = out


def swaps(devices):
    near = [(i, i ^ 1) for i in range(devices)]
    far = [(i, i + 1) for i in range(1, devices - 1, 2)]
    return near, far + [(b, a) for a, b in far]


def exchange(a, b, axis):
    near, far = swaps(lax.axis_size(axis))
    return lax.ppermute(a, axis, near), lax.ppermute(b, axis, far)


def coefficients(m):
    h11, h12, h13, h23, h33 = (m[i] - m[i + 1] for i in range(5))
    h22 = h13

    def inverse(x):
        return jnp.where(x > 0, 1.0 / jnp.where(x > 0, x, 1.0), 0.0)

    d1 = inverse(h11)
    l21, l31 = h12 * d1, h13 * d1
    d2 = inverse(h22 - l21 * h12)
    u23 = h23 - l31 * h12
    l32 = u23 * d2
    d3 = inverse(h33 - l31 * h13 - l32 * u23)
    g1 = m[0]
    g2 = m[1] - l21 * g1
    g3 = m[2] - l31 * g1 - l32 * g2
    c3 = g3 * d3
    c2 = g2 * d2 - l32 * c3
    c1 = g1 * d1 - l21 * c2 - l31 * c3
    return c1, c2, c3


def vmem(n):
    return [pl.BlockSpec(memory_space=pltpu.VMEM)] * n


def shape(*dims):
    return jax.ShapeDtypeStruct(dims, F32)


def params(mib):
    return pltpu.CompilerParams(vmem_limit_bytes=mib << 20)


def per_device(previous, dissipated, material, coolant):
    lasts = TILE // 8 - 1
    edge_specs = []
    for a in (previous, dissipated, material, coolant):
        for at in (0, lasts):
            block = (*a.shape[:-2], 8, TILE)
            edge_specs.append(pl.BlockSpec(block, functools.partial(lambda n, at, i: (0,) * n + (at, 0), a.ndim - 2, at)))
    a, b = pl.pallas_call(
        pack_rows,
        grid=(1,),
        in_specs=edge_specs,
        out_specs=[pl.BlockSpec((FIELDS * HALO, TILE), lambda i: (0, 0))] * 2,
        out_shape=[shape(FIELDS * HALO, TILE)] * 2,
        compiler_params=params(8),
    )(previous, previous, dissipated, dissipated, material, material, coolant, coolant)
    a, b = exchange(a, b, "gx")
    halo, a, b = pl.pallas_call(
        pack_columns,
        in_specs=vmem(6),
        out_specs=vmem(3),
        out_shape=[shape(FIELDS, 8, TILE)] + [shape(TILE + 8, TILE)] * 2,
        compiler_params=params(16),
    )(previous, dissipated, material, coolant, a, b)
    a, b = exchange(a, b, "gy")

    def padded(fields):
        return pltpu.VMEM((fields, ROWS, TILE), F32)

    pairs = SCEN * LAYERS
    w0, w1, w2, moments = pl.pallas_call(
        solve,
        in_specs=vmem(7),
        out_specs=vmem(4),
        out_shape=[shape(pairs, TILE, TILE)] * 3 + [shape(1, TILE)],
        scratch_shapes=[padded(LAYERS)] * 2
        + [padded(pairs)] * 2
        + [padded(FIELDS)]
        + [padded(LAYERS)] * 2
        + [padded(pairs)] * 6,
        compiler_params=params(40),
    )(previous, dissipated, material, coolant, halo, a, b)
    devices = lax.axis_size("gx") * lax.axis_size("gy")
    copies = jnp.broadcast_to(moments, (devices, 1, TILE))
    everything = lax.all_to_all(copies, ("gx", "gy"), split_axis=0, concat_axis=0, tiled=True)
    total = jnp.sum(everything, axis=(0, 1))
    c = coefficients([total[SCEN * i : SCEN * (i + 1)] for i in range(6)])
    c = [x[:, None, None, None] for x in c]
    w0, w1, w2 = (w.reshape(previous.shape) for w in (w0, w1, w2))
    return previous + (c[0] * w0 + c[1] * w1 + c[2] * w2)


def solution(mesh):
    placed = (P(None, None, "gx", "gy"),) * 2 + (P(None, "gx", "gy"),) * 2
    return jax.shard_map(
        per_device, mesh=mesh, in_specs=placed, out_specs=P(None, None, "gx", "gy"), check_vma=False
    )
```

```python
import functools

import jax
import jax.numpy as jnp
from jax import lax
from jax.experimental import pallas as pl
from jax.experimental.pallas import tpu as pltpu
from jax.sharding import PartitionSpec as P

TIER_K = (1.0, 0.3, 0.12, 2.5)
CHANNEL_K = (1.0, 0.3, 0.25, 0.2)
CHANNEL_SINK = (0.0, 0.15, 0.45, 1.2)
TIER_HEAT = 0.05
CHANNEL_HEAT = 0.2
VERTICAL = 4.0

SCEN, TIERS, LAYERS = 2, 4, 7
PAIRS = SCEN * LAYERS
TILE = 128
HALO = 4
GROUP = 16
CHUNKS = TILE // 8
FIELDS = PAIRS + SCEN * TIERS + LAYERS
DISS = PAIRS
CODE = DISS + SCEN * TIERS
MOMENTS = 6
F32 = jnp.float32
ROOT, INVERSE, OVER, LOSS = range(4)


def tables(tier):
    if tier:
        kappa, sink, heat = TIER_K, (0.0,) * 4, TIER_HEAT
    else:
        kappa, sink, heat = CHANNEL_K, CHANNEL_SINK, CHANNEL_HEAT
    root = [k**0.5 for k in kappa]
    return (
        (0.0, *root),
        (0.0, *[1.0 / r for r in root]),
        (1.0, *[(heat + s) / r for s, r in zip(sink, root)]),
        (0.0, *[s / r for s, r in zip(sink, root)]),
    )


def pick(code, table):
    out = jnp.full(code.shape, table[0], F32)
    for index in range(1, 5):
        if table[index] != table[0]:
            out = jnp.where(code == float(index), F32(table[index]), out)
    return out


def pick_inside(code, table):
    out = jnp.full(code.shape, table[4], F32)
    for index in range(1, 4):
        if table[index] != table[4]:
            out = jnp.where(code == float(index), F32(table[index]), out)
    return out


def turn(x, shift, axis=1):
    shift %= x.shape[axis]
    return pltpu.roll(x, shift, axis) if shift else x


def tree(terms):
    while len(terms) > 1:
        terms = [terms[i] + terms[i + 1] if i + 1 < len(terms) else terms[i] for i in range(0, len(terms), 2)]
    return terms[0]


def field_rows(previous, dissipated, material, coolant, field, rows):
    if field < DISS:
        return previous[field // LAYERS, field % LAYERS, rows]
    if field < CODE:
        return dissipated[(field - DISS) // TIERS, (field - DISS) % TIERS, rows]
    layer = field - CODE
    block = material[layer // 2, rows] if layer % 2 == 0 else coolant[layer // 2, rows]
    return block.astype(F32) + 1.0


def pack_rows(prev, diss, mat, cool, a_out, b_out, pt, pb, dt, db, mt, mb, ct, cb, sems):
    copies = []
    for index, (source, top, bottom) in enumerate(((prev, pt, pb), (diss, dt, db), (mat, mt, mb), (cool, ct, cb))):
        lead = (slice(None),) * (len(source.shape) - 2)
        for side, (target, at) in enumerate(((top, 0), (bottom, TILE - 8))):
            copies.append(pltpu.make_async_copy(source.at[(*lead, pl.ds(at, 8))], target, sems.at[2 * index + side]))
    for copy in copies:
        copy.start()
    lower = lax.axis_index("gx") % 2 == 0
    for copy in copies:
        copy.wait()
    for field in range(FIELDS):
        top = field_rows(pt, dt, mt, ct, field, slice(0, HALO))
        bottom = field_rows(pb, db, mb, cb, field, slice(8 - HALO, 8))
        rows = slice(HALO * field, HALO * (field + 1))
        a_out[rows, :] = jnp.where(lower, bottom, top)
        b_out[rows, :] = jnp.where(lower, top, bottom)


def strips_of(get, lane):
    zero = jnp.zeros((8, TILE), F32)
    blocks = []
    for fields in (
        [(layer, layer) for layer in range(LAYERS)],
        [(layer, LAYERS + layer) for layer in range(LAYERS)],
        [(layer, CODE + layer) for layer in range(LAYERS)],
        [(2 * t, DISS + t) for t in range(TIERS)],
        [(2 * t, DISS + TIERS + t) for t in range(TIERS)],
    ):
        out = zero
        for layer, field in fields:
            out = jnp.where(lane // GROUP == layer, turn(get(field), GROUP * layer + 8), out)
        blocks.append(out)
    return blocks


def neighbours(ref, base, r, x):
    out = []
    for layer in range(LAYERS):
        f = base + layer
        t = (ref[f, pl.ds(r - 1, 8), :] + ref[f, pl.ds(r + 1, 8), :]) + (turn(x[layer], 1) + turn(x[layer], -1))
        if layer == 0:
            t = t + VERTICAL * x[1]
        elif layer == LAYERS - 1:
            t = t + VERTICAL * x[layer - 1]
        else:
            t = t + VERTICAL * (x[layer - 1] + x[layer + 1])
        out.append(t)
    return out


def rows_of(ref, base, r, count=LAYERS):
    return [ref[base + i, pl.ds(r, 8), :] for i in range(count)]


def start_field(s, code, x, q, ss, syp, base, diss):
    ys, ts = [], []
    for layer in range(LAYERS):
        t = syp[layer] - (pick(code[layer], tables(False)[LOSS]) + ss[layer] if layer % 2 else ss[layer]) * x[layer]
        if layer % 2 == 0:
            t = t + diss[layer // 2] * pick(code[layer], tables(True)[INVERSE])
        ts.append(t)
        ys.append(q[layer] * t)
    return ys, ts


def begin(prev, diss, mat, cool, c_out, q_out, y0_out, m_out, s_ref, yp_ref):
    lane = lax.broadcasted_iota(jnp.int32, (8, TILE), 1)

    @pl.loop(0, CHUNKS)
    def _(k):
        rows = pl.ds(pl.multiple_of(8 * k, 8), 8)
        inner = pl.ds(pl.multiple_of(8 * k + 8, 8), 8)
        x = [field_rows(prev, diss, mat, cool, f, rows) for f in range(FIELDS)]
        for index, block in enumerate(strips_of(lambda f: x[f], lane)):
            c_out[index, rows, :] = block
        for layer in range(LAYERS):
            s = pick_inside(x[CODE + layer], tables(layer % 2 == 0)[ROOT])
            s_ref[layer, inner, :] = s
            for scen in range(SCEN):
                yp_ref[scen * LAYERS + layer, inner, :] = s * x[scen * LAYERS + layer]

    def body(k, acc):
        rows = pl.ds(pl.multiple_of(8 * k, 8), 8)
        r = pl.multiple_of(8 * k + 8, 8)
        s = rows_of(s_ref, 0, r)
        code = [field_rows(prev, diss, mat, cool, CODE + layer, rows) for layer in range(LAYERS)]
        ss = neighbours(s_ref, 0, r, s)
        q = []
        for layer in range(LAYERS):
            q.append(s[layer] / (pick_inside(code[layer], tables(layer % 2 == 0)[OVER]) + ss[layer]))
            q_out[layer, rows, :] = q[layer]
        sums = []
        for scen in range(SCEN):
            base = scen * LAYERS
            syp = neighbours(yp_ref, base, r, rows_of(yp_ref, base, r))
            x = [prev[scen, layer, rows] for layer in range(LAYERS)]
            d = [diss[scen, t, rows] for t in range(TIERS)]
            y, t = start_field(s, code, x, q, ss, syp, base, d)
            for layer in range(LAYERS):
                y0_out[base + layer, pl.ds(r, 8), :] = y[layer]
            sums.append(tree([a * b for a, b in zip(y, t)]))
        inside = (k > 0) & (k < CHUNKS - 1)
        return tuple(a + jnp.where(inside, b, 0.0) for a, b in zip(acc, sums))

    acc = lax.fori_loop(0, CHUNKS, body, (jnp.zeros((8, TILE), F32),) * SCEN)
    for scen in range(SCEN):
        m_out[scen] = acc[scen]


def messages(c_ref, a_in, b_in, a_out, b_out, halo_out, c_halo):
    lower = lax.axis_index("gx") % 2 == 0
    west = lax.axis_index("gy") % 2 == 0
    lane = lax.broadcasted_iota(jnp.int32, (8, TILE), 1)
    for field in range(FIELDS):
        rows = slice(HALO * field, HALO * (field + 1))
        a, b = a_in[rows, :], b_in[rows, :]
        halo_out[field, :HALO, :] = jnp.where(lower, b, a)
        halo_out[field, HALO:, :] = jnp.where(lower, a, b)
    slot = lane % GROUP // HALO
    odd = lane // GROUP % 2 == 1

    def send(blocks, rows):
        def arrange(base):
            p0, p1, code, d0, d1 = (turn(x, base + HALO * i) for x, i in zip(blocks, (0, 1, 2, 3, 3)))
            d = jnp.where(odd, turn(d1, GROUP), d0)
            return jnp.where(slot < 2, jnp.where(slot == 0, p0, p1), jnp.where(slot == 2, code, d))

        low, high = arrange(-8), arrange(-4)
        a_out[rows, :] = jnp.where(west, high, low)
        b_out[rows, :] = jnp.where(west, low, high)

    for k in range(CHUNKS):
        rows = slice(8 * k, 8 * k + 8)
        send([c_ref[i, rows, :] for i in range(5)], rows)
    blocks = strips_of(lambda f: halo_out[f], lane)
    for index in range(5):
        c_halo[index] = blocks[index]
    send(blocks, slice(TILE, TILE + 8))


def middle(prev, diss, mat, cool, halo, q_ref, y0, m_in, y1, y2, y0_fix, m_out, sn, ypn, y0n, y1n, y2n):
    zero = jnp.zeros((8, TILE), F32)

    def sweep(x_ref, out_ref):
        def body(k, acc):
            rows = pl.ds(pl.multiple_of(8 * k, 8), 8)
            r = pl.multiple_of(8 * k + 8, 8)
            odd, even = [], []
            for scen in range(SCEN):
                base = scen * LAYERS
                x = rows_of(x_ref, base, r)
                t = neighbours(x_ref, base, r, x)
                odd.append(tree([a * b for a, b in zip(x, t)]))
                if out_ref is not None:
                    p = []
                    for layer in range(LAYERS):
                        y = q_ref[layer, rows, :] * t[layer]
                        out_ref[base + layer, pl.ds(r, 8), :] = y
                        p.append(y * t[layer])
                    even.append(tree(p))
            inside = (k > 0) & (k < CHUNKS - 1)
            return tuple(a + jnp.where(inside, b, 0.0) for a, b in zip(acc, odd + even))

        return lax.fori_loop(0, CHUNKS, body, (zero,) * (SCEN if out_ref is None else 2 * SCEN))

    m = [m_in[scen] for scen in range(SCEN)]
    m += sweep(y0, y1)
    m += sweep(y1, y2)
    m += sweep(y2, None)

    for side in range(2):
        own = 16 if side == 0 else 8
        beyond = 24 - own
        near = slice(0, 8) if side == 0 else slice(TILE - 8, TILE)
        inner = slice(8, 16) if side == 0 else slice(TILE - 16, TILE - 8)
        inner_at = 24 if side == 0 else 0
        chunks = (
            (own, lambda f: field_rows(prev, diss, mat, cool, f, near)),
            (inner_at, lambda f: field_rows(prev, diss, mat, cool, f, inner)),
            (beyond, lambda f: turn(halo[f], 4, 0)),
        )
        for at, get in chunks:
            for layer in range(LAYERS):
                s = pick(get(CODE + layer), tables(layer % 2 == 0)[ROOT])
                sn[layer, at : at + 8, :] = s
                for scen in range(SCEN):
                    ypn[scen * LAYERS + layer, at : at + 8, :] = s * get(scen * LAYERS + layer)
        padded_inner = slice(inner.start + 8, inner.stop + 8)
        padded_near = slice(near.start + 8, near.stop + 8)
        fix = slice(8 * side, 8 * side + 8)
        for f in range(PAIRS):
            y0n[f, inner_at : inner_at + 8, :] = y0[f, padded_inner, :]
            y1n[f, inner_at : inner_at + 8, :] = y1[f, padded_inner, :]
            y2n[f, inner_at : inner_at + 8, :] = y2[f, padded_inner, :]
        q = {}
        for at, get in (chunks[0], chunks[2]):
            s = rows_of(sn, 0, at)
            ss = neighbours(sn, 0, at, s)
            code = [get(CODE + layer) for layer in range(LAYERS)]
            q[at] = [s[i] / (pick(code[i], tables(i % 2 == 0)[OVER]) + ss[i]) for i in range(LAYERS)]
            for scen in range(SCEN):
                base = scen * LAYERS
                syp = neighbours(ypn, base, at, rows_of(ypn, base, at))
                x = [get(base + layer) for layer in range(LAYERS)]
                d = [get(DISS + scen * TIERS + t) for t in range(TIERS)]
                y, t = start_field(s, code, x, q[at], ss, syp, base, d)
                for layer in range(LAYERS):
                    y0n[base + layer, at : at + 8, :] = y[layer]
                    if at == own:
                        y0_fix[base + layer, fix, :] = y[layer]
                if at == own:
                    m[scen] = m[scen] + tree([a * b for a, b in zip(y, t)])
        for level, (x_ref, n_ref, out_ref) in enumerate(((y0n, y1n, y1), (y1n, y2n, y2), (y2n, None, None))):
            for at in (own, beyond) if n_ref is not None else (own,):
                for scen in range(SCEN):
                    base = scen * LAYERS
                    x = rows_of(x_ref, base, at)
                    t = neighbours(x_ref, base, at, x)
                    if at == own:
                        index = SCEN * (2 * level + 1) + scen
                        m[index] = m[index] + tree([a * b for a, b in zip(x, t)])
                    if n_ref is None:
                        continue
                    p = []
                    for layer in range(LAYERS):
                        y = q[at][layer] * t[layer]
                        n_ref[base + layer, at : at + 8, :] = y
                        if at == own:
                            out_ref[base + layer, padded_near, :] = y
                            p.append(y * t[layer])
                    if at == own:
                        index = SCEN * (2 * level + 2) + scen
                        m[index] = m[index] + tree(p)
    for index in range(SCEN * MOMENTS):
        m_out[index] = m[index]


TOP = 16
ROWS = TOP + TILE + 16


def strips(c_ref, c_halo, a_in, b_in, m_in, ys_out, m_out, code_ref, s_ref, x_ref, d_ref, yp_ref, q_ref, y0, y1, y2):
    west = lax.axis_index("gy") % 2 == 0
    lane = lax.broadcasted_iota(jnp.int32, (8, TILE), 1)
    place = lane % GROUP
    real = lane < GROUP * LAYERS
    tier = lane // GROUP % 2 == 0
    zero = jnp.zeros((8, TILE), F32)
    sides = (
        (place < 8, (place >= 8) & (place < 12) & real, (place >= 4) & (place < 8) & real, 8),
        (place >= 8, (place >= 4) & (place < 8) & real, (place >= 8) & (place < 12) & real, 4),
    )

    def lookup(code, kind):
        out = zero if tables(True)[kind][0] == 0.0 else jnp.full_like(zero, tables(True)[kind][0])
        for index in range(1, 5):
            value = jnp.where(tier, F32(tables(True)[kind][index]), F32(tables(False)[kind][index]))
            out = jnp.where(code == float(index), value, out)
        return out

    chunk_rows = [(slice(8 * k, 8 * k + 8), (8 * k + TOP,), 0) for k in range(CHUNKS)]
    chunk_rows.append((None, (TOP - 8, TOP + TILE), 4))
    for rows, targets, rotation in chunk_rows:
        message = slice(TILE, TILE + 8) if rows is None else rows
        a, b = a_in[message, :], b_in[message, :]
        blocks = [c_halo[i] if rows is None else c_ref[i, rows, :] for i in range(5)]
        for side, (own, beyond, _, base) in enumerate(sides):
            got = jnp.where(west, a, b) if side == 0 else jnp.where(west, b, a)
            full = []
            for index, shift in enumerate((base, base - 4, base - 8, base - 12, base - 12 - GROUP)):
                mask = beyond if index < 3 else beyond & tier
                full.append(jnp.where(own, blocks[index], jnp.where(mask, turn(got, shift), zero)))
            full = [turn(x, rotation, 0) for x in full]
            s = lookup(full[2], ROOT)
            for at in targets:
                here = slice(at, at + 8)
                code_ref[side, here, :] = full[2]
                s_ref[side, here, :] = s
                for scen in range(SCEN):
                    x_ref[2 * scen + side, here, :] = full[scen]
                    d_ref[2 * scen + side, here, :] = full[3 + scen]
                    yp_ref[2 * scen + side, here, :] = s * full[scen]

    def around(ref, index, at):
        x = ref[index, at : at + 8, :]
        lateral = (ref[index, at - 1 : at + 7, :] + ref[index, at + 1 : at + 9, :]) + (turn(x, 1) + turn(x, -1))
        return x, lateral + VERTICAL * (turn(x, GROUP) + turn(x, -GROUP))

    everywhere = range(TOP - 8, TOP + TILE + 8, 8)
    within = range(TOP, TOP + TILE, 8)
    m = [[zero, zero] for _ in range(SCEN * MOMENTS)]

    def count(index, side, at, value):
        if at in within:
            m[index][side] = m[index][side] + value

    for at in everywhere:
        here = slice(at, at + 8)
        for side in range(2):
            code = code_ref[side, here, :]
            s, ss = around(s_ref, side, at)
            q = s / (lookup(code, OVER) + ss)
            q_ref[side, here, :] = q
            inverse, loss = lookup(code, INVERSE), lookup(code, LOSS) + ss
            for scen in range(SCEN):
                f = 2 * scen + side
                _, syp = around(yp_ref, f, at)
                t = syp - loss * x_ref[f, here, :] + d_ref[f, here, :] * inverse
                y = q * t
                y0[f, here, :] = y
                count(scen, side, at, y * t)
    for level, (ref, out) in enumerate(((y0, y1), (y1, y2), (y2, None))):
        for at in everywhere if out is not None else within:
            here = slice(at, at + 8)
            for side in range(2):
                for scen in range(SCEN):
                    f = 2 * scen + side
                    x, t = around(ref, f, at)
                    count(SCEN * (2 * level + 1) + scen, side, at, x * t)
                    if out is not None:
                        y = q_ref[side, here, :] * t
                        out[f, here, :] = y
                        count(SCEN * (2 * level + 2) + scen, side, at, y * t)
    for level, ref in enumerate((y0, y1, y2)):
        for scen in range(SCEN):
            for k in range(CHUNKS):
                here = slice(8 * k + TOP, 8 * k + TOP + 8)
                merged = jnp.where(place < 8, ref[2 * scen, here, :], ref[2 * scen + 1, here, :])
                ys_out[SCEN * level + scen, 8 * k : 8 * k + 8, :] = merged
    line = lax.broadcasted_iota(jnp.int32, (8, TILE), 1)
    inner = (lane >= HALO) & (lane < TILE - HALO)
    out = zero
    for index in range(SCEN * MOMENTS):
        east, wst = (jnp.where(sides[side][2], m[index][side], 0.0) for side in range(2))
        value = jnp.where(inner, m_in[index], 0.0) + (east + wst)
        value = jnp.sum(jnp.sum(value, axis=0, keepdims=True), axis=1, keepdims=True)
        out = jnp.where(line == index, value, out)
    m_out[...] = jnp.broadcast_to(out, m_out.shape)


def combine(prev, mat, cool, y0, y0_fix, y1, y2, ys, m_ref, out, buffer, sems):
    lane = lax.broadcasted_iota(jnp.int32, (8, TILE), 1)
    edge = (lane < HALO) | (lane >= TILE - HALO)
    total = tree([m_ref[i] for i in range(m_ref.shape[0])])
    total = jnp.broadcast_to(jnp.sum(total, axis=0, keepdims=True), (8, TILE))
    weights = coefficients([turn(total, -SCEN * i) for i in range(MOMENTS)])
    c = [
        [jnp.broadcast_to(jnp.sum(jnp.where(lane == scen, w, 0.0), axis=1, keepdims=True), (8, TILE)) for w in weights]
        for scen in range(SCEN)
    ]
    parts = 4
    copies = []

    def chunk(k, at, first):
        rows = pl.ds(at, 8)
        padded = pl.ds(at + 8, 8)
        scale = [
            pick_inside(field_rows(prev, None, mat, cool, CODE + layer, rows), tables(layer % 2 == 0)[INVERSE])
            for layer in range(LAYERS)
        ]
        for scen in range(SCEN):
            strip = tree([c[scen][i] * ys[SCEN * i + scen, rows, :] for i in range(3)])
            for layer in range(LAYERS):
                f = scen * LAYERS + layer
                value = c[scen][1] * y1[f, padded, :] + c[scen][2] * y2[f, padded, :] + c[scen][0] * first(f)
                value = jnp.where(edge, turn(strip, 120 - GROUP * layer), value)
                buffer[scen, layer, rows, :] = prev[scen, layer, rows] + scale[layer] * value

    for part in range(parts):
        if part == 0:
            chunk(0, 0, lambda f: y0_fix[f, 0:8, :])
        low = max(1, part * CHUNKS // parts)
        high = min(CHUNKS - 1, (part + 1) * CHUNKS // parts)

        @pl.loop(low, high)
        def _(k):
            at = pl.multiple_of(8 * k, 8)
            chunk(k, at, lambda f: y0[f, pl.ds(at + 8, 8), :])

        if part == parts - 1:
            chunk(CHUNKS - 1, TILE - 8, lambda f: y0_fix[f, 8:16, :])
        rows = pl.ds(part * TILE // parts, TILE // parts)
        copy = pltpu.make_async_copy(buffer.at[:, :, rows], out.at[:, :, rows], sems.at[part])
        copy.start()
        copies.append(copy)
    for copy in copies:
        copy.wait()


def swaps(devices):
    near = [(i, i ^ 1) for i in range(devices)]
    far = [(i, i + 1) for i in range(1, devices - 1, 2)]
    return near, far + [(b, a) for a, b in far]


def exchange(a, b, axis):
    near, far = swaps(lax.axis_size(axis))
    return lax.ppermute(a, axis, near), lax.ppermute(b, axis, far)


def coefficients(m):
    h11, h12, h13, h23, h33 = (m[i] - m[i + 1] for i in range(5))
    h22 = h13

    def inverse(x):
        return jnp.where(x > 0, 1.0 / jnp.where(x > 0, x, 1.0), 0.0)

    d1 = inverse(h11)
    l21, l31 = h12 * d1, h13 * d1
    d2 = inverse(h22 - l21 * h12)
    u23 = h23 - l31 * h12
    l32 = u23 * d2
    d3 = inverse(h33 - l31 * h13 - l32 * u23)
    g1 = m[0]
    g2 = m[1] - l21 * g1
    g3 = m[2] - l31 * g1 - l32 * g2
    c3 = g3 * d3
    c2 = g2 * d2 - l32 * c3
    c1 = g1 * d1 - l21 * c2 - l31 * c3
    return c1, c2, c3


def vmem(n):
    return [pl.BlockSpec(memory_space=pltpu.VMEM)] * n


def shape(*dims):
    return jax.ShapeDtypeStruct(dims, F32)


def call(kernel, inputs, outputs, scratch, mib, flops, in_specs=None, out_specs=None):
    many = isinstance(outputs, list)
    return pl.pallas_call(
        kernel,
        in_specs=in_specs or vmem(len(inputs)),
        out_specs=out_specs or (vmem(len(outputs)) if many else vmem(1)[0]),
        out_shape=outputs,
        scratch_shapes=scratch,
        compiler_params=pltpu.CompilerParams(vmem_limit_bytes=int(mib * 2**20)),
        cost_estimate=pl.CostEstimate(flops=flops, bytes_accessed=1 << 20, transcendentals=0),
    )(*inputs)


def per_device(previous, dissipated, material, coolant):
    given = (previous, dissipated, material, coolant)

    def buffer(dtype, *dims):
        return pltpu.VMEM(dims, dtype)

    edges = []
    for a in given:
        edges += [buffer(a.dtype, *a.shape[:-2], 8, TILE)] * 2
    a, b = call(
        pack_rows,
        given,
        [shape(FIELDS * HALO, TILE)] * 2,
        edges + [pltpu.SemaphoreType.DMA((8,))],
        62,
        1 << 20,
        in_specs=[pl.BlockSpec(memory_space=pltpu.HBM)] * 4,
    )
    a, b = exchange(a, b, "gx")
    padded = TILE + 16
    c_blocks, q, y0, m0 = call(
        begin,
        given,
        [shape(5, TILE, TILE), shape(LAYERS, TILE, TILE), shape(PAIRS, padded, TILE), shape(SCEN, 8, TILE)],
        [buffer(F32, LAYERS, padded, TILE), buffer(F32, PAIRS, padded, TILE)],
        8,
        1 << 27,
    )
    a, b, halo, c_halo = call(
        messages,
        (c_blocks, a, b),
        [shape(TILE + 8, TILE)] * 2 + [shape(FIELDS, 8, TILE), shape(5, 8, TILE)],
        [],
        4,
        1 << 20,
    )
    a, b = exchange(a, b, "gy")
    y1, y2, y0_fix, m = call(
        middle,
        (*given, halo, q, y0, m0),
        [shape(PAIRS, padded, TILE)] * 2 + [shape(PAIRS, 16, TILE), shape(SCEN * MOMENTS, 8, TILE)],
        [buffer(F32, LAYERS, 32, TILE)] + [buffer(F32, PAIRS, 32, TILE)] * 4,
        8,
        1 << 27,
    )
    devices = lax.axis_size("gx") * lax.axis_size("gy")
    ys, m = call(
        strips,
        (c_blocks, c_halo, a, b, m),
        [shape(3 * SCEN, TILE, TILE), shape(devices // 8, 8, TILE)],
        [buffer(F32, n, ROWS, TILE) for n in (2, 2, 4, 4, 4, 2, 4, 4, 4)],
        8,
        1 << 24,
    )
    everything = lax.all_to_all(m.reshape(devices, 1, TILE), ("gx", "gy"), split_axis=0, concat_axis=0, tiled=True)
    return call(
        combine,
        (previous, material, coolant, y0, y0_fix, y1, y2, ys, everything.reshape(devices // 8, 8, TILE)),
        shape(*previous.shape),
        [buffer(F32, *previous.shape), pltpu.SemaphoreType.DMA((4,))],
        8,
        1 << 24,
        out_specs=pl.BlockSpec(memory_space=pltpu.HBM),
    )


def solution(mesh):
    placed = (P(None, None, "gx", "gy"),) * 2 + (P(None, "gx", "gy"),) * 2
    return jax.shard_map(
        per_device, mesh=mesh, in_specs=placed, out_specs=P(None, None, "gx", "gy"), check_vma=False
    )
```

```python
import functools

import jax
import jax.numpy as jnp
from jax import lax
from jax.experimental import pallas as pl
from jax.experimental.pallas import tpu as pltpu
from jax.sharding import PartitionSpec as P

TIER_K = (1.0, 0.3, 0.12, 2.5)
CHANNEL_K = (1.0, 0.3, 0.25, 0.2)
CHANNEL_SINK = (0.0, 0.15, 0.45, 1.2)
TIER_HEAT = 0.05
CHANNEL_HEAT = 0.2
VERTICAL = 4.0

SCEN, TIERS, LAYERS = 2, 4, 7
PAIRS = SCEN * LAYERS
TILE = 128
HALO = 4
GROUP = 16
CHUNKS = TILE // 8
FIELDS = PAIRS + SCEN * TIERS + LAYERS
DISS = PAIRS
CODE = DISS + SCEN * TIERS
MOMENTS = 6
F32 = jnp.float32
ROOT, INVERSE, OVER, LOSS = range(4)


def tables(tier):
    if tier:
        kappa, sink, heat = TIER_K, (0.0,) * 4, TIER_HEAT
    else:
        kappa, sink, heat = CHANNEL_K, CHANNEL_SINK, CHANNEL_HEAT
    root = [k**0.5 for k in kappa]
    return (
        (0.0, *root),
        (0.0, *[1.0 / r for r in root]),
        (1.0, *[(heat + s) / r for s, r in zip(sink, root)]),
        (0.0, *[s / r for s, r in zip(sink, root)]),
    )


def pick(code, table):
    out = jnp.full(code.shape, table[0], F32)
    for index in range(1, 5):
        if table[index] != table[0]:
            out = jnp.where(code == float(index), F32(table[index]), out)
    return out


def pick_inside(code, table):
    out = jnp.full(code.shape, table[4], F32)
    for index in range(1, 4):
        if table[index] != table[4]:
            out = jnp.where(code == float(index), F32(table[index]), out)
    return out


def turn(x, shift, axis=1):
    shift %= x.shape[axis]
    return pltpu.roll(x, shift, axis) if shift else x


def tree(terms):
    while len(terms) > 1:
        terms = [terms[i] + terms[i + 1] if i + 1 < len(terms) else terms[i] for i in range(0, len(terms), 2)]
    return terms[0]


def field_rows(previous, dissipated, material, coolant, field, rows):
    if field < DISS:
        return previous[field // LAYERS, field % LAYERS, rows]
    if field < CODE:
        return dissipated[(field - DISS) // TIERS, (field - DISS) % TIERS, rows]
    layer = field - CODE
    block = material[layer // 2, rows] if layer % 2 == 0 else coolant[layer // 2, rows]
    return block.astype(F32) + 1.0


def pack_rows(prev, diss, mat, cool, a_out, b_out, pt, pb, dt, db, mt, mb, ct, cb, sems):
    copies = []
    for index, (source, top, bottom) in enumerate(((prev, pt, pb), (diss, dt, db), (mat, mt, mb), (cool, ct, cb))):
        lead = (slice(None),) * (len(source.shape) - 2)
        for side, (target, at) in enumerate(((top, 0), (bottom, TILE - 8))):
            copies.append(pltpu.make_async_copy(source.at[(*lead, pl.ds(at, 8))], target, sems.at[2 * index + side]))
    for copy in copies:
        copy.start()
    lower = lax.axis_index("gx") % 2 == 0
    for copy in copies:
        copy.wait()
    for field in range(FIELDS):
        top = field_rows(pt, dt, mt, ct, field, slice(0, HALO))
        bottom = field_rows(pb, db, mb, cb, field, slice(8 - HALO, 8))
        rows = slice(HALO * field, HALO * (field + 1))
        a_out[rows, :] = jnp.where(lower, bottom, top)
        b_out[rows, :] = jnp.where(lower, top, bottom)


def strips_of(get, lane):
    zero = jnp.zeros((8, TILE), F32)
    blocks = []
    for fields in (
        [(layer, layer) for layer in range(LAYERS)],
        [(layer, LAYERS + layer) for layer in range(LAYERS)],
        [(layer, CODE + layer) for layer in range(LAYERS)],
        [(2 * t, DISS + t) for t in range(TIERS)],
        [(2 * t, DISS + TIERS + t) for t in range(TIERS)],
    ):
        out = zero
        for layer, field in fields:
            out = jnp.where(lane // GROUP == layer, turn(get(field), GROUP * layer + 8), out)
        blocks.append(out)
    return blocks


def neighbours(ref, base, r, x):
    out = []
    for layer in range(LAYERS):
        f = base + layer
        t = (ref[f, pl.ds(r - 1, 8), :] + ref[f, pl.ds(r + 1, 8), :]) + (turn(x[layer], 1) + turn(x[layer], -1))
        if layer == 0:
            t = t + VERTICAL * x[1]
        elif layer == LAYERS - 1:
            t = t + VERTICAL * x[layer - 1]
        else:
            t = t + VERTICAL * (x[layer - 1] + x[layer + 1])
        out.append(t)
    return out


def rows_of(ref, base, r, count=LAYERS):
    return [ref[base + i, pl.ds(r, 8), :] for i in range(count)]


def start_field(s, code, x, q, ss, syp, base, diss):
    ys, ts = [], []
    for layer in range(LAYERS):
        t = syp[layer] - (pick(code[layer], tables(False)[LOSS]) + ss[layer] if layer % 2 else ss[layer]) * x[layer]
        if layer % 2 == 0:
            t = t + diss[layer // 2] * pick(code[layer], tables(True)[INVERSE])
        ts.append(t)
        ys.append(q[layer] * t)
    return ys, ts


def begin(prev, diss, mat, cool, c_out, q_out, y0_out, m_out, s_ref, yp_ref):
    lane = lax.broadcasted_iota(jnp.int32, (8, TILE), 1)

    for k in range(CHUNKS):
        rows = slice(8 * k, 8 * k + 8)
        inner = slice(8 * k + 8, 8 * k + 16)
        x = [field_rows(prev, diss, mat, cool, f, rows) for f in range(FIELDS)]
        for index, block in enumerate(strips_of(lambda f: x[f], lane)):
            c_out[index, rows, :] = block
        for layer in range(LAYERS):
            s = pick_inside(x[CODE + layer], tables(layer % 2 == 0)[ROOT])
            s_ref[layer, inner, :] = s
            for scen in range(SCEN):
                yp_ref[scen * LAYERS + layer, inner, :] = s * x[scen * LAYERS + layer]

    acc = [jnp.zeros((8, TILE), F32)] * SCEN
    for k in range(CHUNKS):
        rows = slice(8 * k, 8 * k + 8)
        r = 8 * k + 8
        s = rows_of(s_ref, 0, r)
        code = [field_rows(prev, diss, mat, cool, CODE + layer, rows) for layer in range(LAYERS)]
        ss = neighbours(s_ref, 0, r, s)
        q = []
        for layer in range(LAYERS):
            q.append(s[layer] / (pick_inside(code[layer], tables(layer % 2 == 0)[OVER]) + ss[layer]))
            q_out[layer, rows, :] = q[layer]
        sums = []
        for scen in range(SCEN):
            base = scen * LAYERS
            syp = neighbours(yp_ref, base, r, rows_of(yp_ref, base, r))
            x = [prev[scen, layer, rows] for layer in range(LAYERS)]
            d = [diss[scen, t, rows] for t in range(TIERS)]
            y, t = start_field(s, code, x, q, ss, syp, base, d)
            for layer in range(LAYERS):
                y0_out[base + layer, pl.ds(r, 8), :] = y[layer]
            sums.append(tree([a * b for a, b in zip(y, t)]))
        if 0 < k < CHUNKS - 1:
            acc = [a + b for a, b in zip(acc, sums)]
    for scen in range(SCEN):
        m_out[scen] = acc[scen]


def messages(c_ref, a_in, b_in, a_out, b_out, halo_out, c_halo):
    lower = lax.axis_index("gx") % 2 == 0
    west = lax.axis_index("gy") % 2 == 0
    lane = lax.broadcasted_iota(jnp.int32, (8, TILE), 1)
    for field in range(FIELDS):
        rows = slice(HALO * field, HALO * (field + 1))
        a, b = a_in[rows, :], b_in[rows, :]
        halo_out[field, :HALO, :] = jnp.where(lower, b, a)
        halo_out[field, HALO:, :] = jnp.where(lower, a, b)
    slot = lane % GROUP // HALO
    odd = lane // GROUP % 2 == 1

    def send(blocks, rows):
        def arrange(base):
            p0, p1, code, d0, d1 = (turn(x, base + HALO * i) for x, i in zip(blocks, (0, 1, 2, 3, 3)))
            d = jnp.where(odd, turn(d1, GROUP), d0)
            return jnp.where(slot < 2, jnp.where(slot == 0, p0, p1), jnp.where(slot == 2, code, d))

        low, high = arrange(-8), arrange(-4)
        a_out[rows, :] = jnp.where(west, high, low)
        b_out[rows, :] = jnp.where(west, low, high)

    for k in range(CHUNKS):
        rows = slice(8 * k, 8 * k + 8)
        send([c_ref[i, rows, :] for i in range(5)], rows)
    blocks = strips_of(lambda f: halo_out[f], lane)
    for index in range(5):
        c_halo[index] = blocks[index]
    send(blocks, slice(TILE, TILE + 8))


def middle(prev, diss, mat, cool, halo, q_ref, y0, m_in, y1, y2, y0_fix, m_out, sn, ypn, y0n, y1n, y2n):
    zero = jnp.zeros((8, TILE), F32)

    def sweep(x_ref, out_ref):
        acc = [zero] * (SCEN if out_ref is None else 2 * SCEN)
        for k in range(CHUNKS):
            if out_ref is None and k in (0, CHUNKS - 1):
                continue
            rows = slice(8 * k, 8 * k + 8)
            r = 8 * k + 8
            odd, even = [], []
            for scen in range(SCEN):
                base = scen * LAYERS
                x = rows_of(x_ref, base, r)
                t = neighbours(x_ref, base, r, x)
                odd.append(tree([a * b for a, b in zip(x, t)]))
                if out_ref is not None:
                    p = []
                    for layer in range(LAYERS):
                        y = q_ref[layer, rows, :] * t[layer]
                        out_ref[base + layer, pl.ds(r, 8), :] = y
                        p.append(y * t[layer])
                    even.append(tree(p))
            if 0 < k < CHUNKS - 1:
                acc = [a + b for a, b in zip(acc, odd + even)]
        return acc

    m = [m_in[scen] for scen in range(SCEN)]
    m += sweep(y0, y1)
    m += sweep(y1, y2)
    m += sweep(y2, None)

    for side in range(2):
        own = 16 if side == 0 else 8
        beyond = 24 - own
        near = slice(0, 8) if side == 0 else slice(TILE - 8, TILE)
        inner = slice(8, 16) if side == 0 else slice(TILE - 16, TILE - 8)
        inner_at = 24 if side == 0 else 0
        chunks = (
            (own, lambda f: field_rows(prev, diss, mat, cool, f, near)),
            (inner_at, lambda f: field_rows(prev, diss, mat, cool, f, inner)),
            (beyond, lambda f: turn(halo[f], 4, 0)),
        )
        for at, get in chunks:
            for layer in range(LAYERS):
                s = pick(get(CODE + layer), tables(layer % 2 == 0)[ROOT])
                sn[layer, at : at + 8, :] = s
                for scen in range(SCEN):
                    ypn[scen * LAYERS + layer, at : at + 8, :] = s * get(scen * LAYERS + layer)
        padded_inner = slice(inner.start + 8, inner.stop + 8)
        padded_near = slice(near.start + 8, near.stop + 8)
        fix = slice(8 * side, 8 * side + 8)
        for f in range(PAIRS):
            y0n[f, inner_at : inner_at + 8, :] = y0[f, padded_inner, :]
            y1n[f, inner_at : inner_at + 8, :] = y1[f, padded_inner, :]
            y2n[f, inner_at : inner_at + 8, :] = y2[f, padded_inner, :]
        q = {}
        for at, get in (chunks[0], chunks[2]):
            s = rows_of(sn, 0, at)
            ss = neighbours(sn, 0, at, s)
            code = [get(CODE + layer) for layer in range(LAYERS)]
            q[at] = [s[i] / (pick(code[i], tables(i % 2 == 0)[OVER]) + ss[i]) for i in range(LAYERS)]
            for scen in range(SCEN):
                base = scen * LAYERS
                syp = neighbours(ypn, base, at, rows_of(ypn, base, at))
                x = [get(base + layer) for layer in range(LAYERS)]
                d = [get(DISS + scen * TIERS + t) for t in range(TIERS)]
                y, t = start_field(s, code, x, q[at], ss, syp, base, d)
                for layer in range(LAYERS):
                    y0n[base + layer, at : at + 8, :] = y[layer]
                    if at == own:
                        y0_fix[base + layer, fix, :] = y[layer]
                if at == own:
                    m[scen] = m[scen] + tree([a * b for a, b in zip(y, t)])
        for level, (x_ref, n_ref, out_ref) in enumerate(((y0n, y1n, y1), (y1n, y2n, y2), (y2n, None, None))):
            for at in (own, beyond) if n_ref is not None else (own,):
                for scen in range(SCEN):
                    base = scen * LAYERS
                    x = rows_of(x_ref, base, at)
                    t = neighbours(x_ref, base, at, x)
                    if at == own:
                        index = SCEN * (2 * level + 1) + scen
                        m[index] = m[index] + tree([a * b for a, b in zip(x, t)])
                    if n_ref is None:
                        continue
                    p = []
                    for layer in range(LAYERS):
                        y = q[at][layer] * t[layer]
                        n_ref[base + layer, at : at + 8, :] = y
                        if at == own:
                            out_ref[base + layer, padded_near, :] = y
                            p.append(y * t[layer])
                    if at == own:
                        index = SCEN * (2 * level + 2) + scen
                        m[index] = m[index] + tree(p)
    for index in range(SCEN * MOMENTS):
        m_out[index] = m[index]


TOP = 16
ROWS = TOP + TILE + 16


def strips(c_ref, c_halo, a_in, b_in, m_in, ys_out, m_out, code_ref, s_ref, x_ref, d_ref, yp_ref, q_ref, y0, y1, y2):
    west = lax.axis_index("gy") % 2 == 0
    lane = lax.broadcasted_iota(jnp.int32, (8, TILE), 1)
    place = lane % GROUP
    real = lane < GROUP * LAYERS
    tier = lane // GROUP % 2 == 0
    zero = jnp.zeros((8, TILE), F32)
    sides = (
        (place < 8, (place >= 8) & (place < 12) & real, (place >= 4) & (place < 8) & real, 8),
        (place >= 8, (place >= 4) & (place < 8) & real, (place >= 8) & (place < 12) & real, 4),
    )

    def lookup(code, kind):
        out = zero if tables(True)[kind][0] == 0.0 else jnp.full_like(zero, tables(True)[kind][0])
        for index in range(1, 5):
            value = jnp.where(tier, F32(tables(True)[kind][index]), F32(tables(False)[kind][index]))
            out = jnp.where(code == float(index), value, out)
        return out

    chunk_rows = [(slice(8 * k, 8 * k + 8), (8 * k + TOP,), 0) for k in range(CHUNKS)]
    chunk_rows.append((None, (TOP - 8, TOP + TILE), 4))
    for rows, targets, rotation in chunk_rows:
        message = slice(TILE, TILE + 8) if rows is None else rows
        a, b = a_in[message, :], b_in[message, :]
        blocks = [c_halo[i] if rows is None else c_ref[i, rows, :] for i in range(5)]
        for side, (own, beyond, _, base) in enumerate(sides):
            got = jnp.where(west, a, b) if side == 0 else jnp.where(west, b, a)
            full = []
            for index, shift in enumerate((base, base - 4, base - 8, base - 12, base - 12 - GROUP)):
                mask = beyond if index < 3 else beyond & tier
                full.append(jnp.where(own, blocks[index], jnp.where(mask, turn(got, shift), zero)))
            full = [turn(x, rotation, 0) for x in full]
            s = lookup(full[2], ROOT)
            for at in targets:
                here = slice(at, at + 8)
                code_ref[side, here, :] = full[2]
                s_ref[side, here, :] = s
                for scen in range(SCEN):
                    x_ref[2 * scen + side, here, :] = full[scen]
                    d_ref[2 * scen + side, here, :] = full[3 + scen]
                    yp_ref[2 * scen + side, here, :] = s * full[scen]

    def around(ref, index, at):
        x = ref[index, at : at + 8, :]
        lateral = (ref[index, at - 1 : at + 7, :] + ref[index, at + 1 : at + 9, :]) + (turn(x, 1) + turn(x, -1))
        return x, lateral + VERTICAL * (turn(x, GROUP) + turn(x, -GROUP))

    everywhere = range(TOP - 8, TOP + TILE + 8, 8)
    within = range(TOP, TOP + TILE, 8)
    m = [[zero, zero] for _ in range(SCEN * MOMENTS)]

    def count(index, side, at, value):
        if at in within:
            m[index][side] = m[index][side] + value

    for at in everywhere:
        here = slice(at, at + 8)
        for side in range(2):
            code = code_ref[side, here, :]
            s, ss = around(s_ref, side, at)
            q = s / (lookup(code, OVER) + ss)
            q_ref[side, here, :] = q
            inverse, loss = lookup(code, INVERSE), lookup(code, LOSS) + ss
            for scen in range(SCEN):
                f = 2 * scen + side
                _, syp = around(yp_ref, f, at)
                t = syp - loss * x_ref[f, here, :] + d_ref[f, here, :] * inverse
                y = q * t
                y0[f, here, :] = y
                count(scen, side, at, y * t)
    for level, (ref, out) in enumerate(((y0, y1), (y1, y2), (y2, None))):
        for at in everywhere if out is not None else within:
            here = slice(at, at + 8)
            for side in range(2):
                for scen in range(SCEN):
                    f = 2 * scen + side
                    x, t = around(ref, f, at)
                    count(SCEN * (2 * level + 1) + scen, side, at, x * t)
                    if out is not None:
                        y = q_ref[side, here, :] * t
                        out[f, here, :] = y
                        count(SCEN * (2 * level + 2) + scen, side, at, y * t)
    for level, ref in enumerate((y0, y1, y2)):
        for scen in range(SCEN):
            for k in range(CHUNKS):
                here = slice(8 * k + TOP, 8 * k + TOP + 8)
                merged = jnp.where(place < 8, ref[2 * scen, here, :], ref[2 * scen + 1, here, :])
                ys_out[SCEN * level + scen, 8 * k : 8 * k + 8, :] = merged
    line = lax.broadcasted_iota(jnp.int32, (8, TILE), 1)
    inner = (lane >= HALO) & (lane < TILE - HALO)
    out = zero
    for index in range(SCEN * MOMENTS):
        east, wst = (jnp.where(sides[side][2], m[index][side], 0.0) for side in range(2))
        value = jnp.where(inner, m_in[index], 0.0) + (east + wst)
        value = jnp.sum(jnp.sum(value, axis=0, keepdims=True), axis=1, keepdims=True)
        out = jnp.where(line == index, value, out)
    m_out[...] = jnp.broadcast_to(out, m_out.shape)


def combine(prev, mat, cool, y0, y0_fix, y1, y2, ys, m_ref, out, buffer, sems):
    lane = lax.broadcasted_iota(jnp.int32, (8, TILE), 1)
    edge = (lane < HALO) | (lane >= TILE - HALO)
    total = tree([m_ref[i] for i in range(m_ref.shape[0])])
    total = jnp.broadcast_to(jnp.sum(total, axis=0, keepdims=True), (8, TILE))
    weights = coefficients([turn(total, -SCEN * i) for i in range(MOMENTS)])
    c = [
        [jnp.broadcast_to(jnp.sum(jnp.where(lane == scen, w, 0.0), axis=1, keepdims=True), (8, TILE)) for w in weights]
        for scen in range(SCEN)
    ]
    parts = 4
    copies = []

    def chunk(k, at, first):
        rows = pl.ds(at, 8)
        padded = pl.ds(at + 8, 8)
        scale = [
            pick_inside(field_rows(prev, None, mat, cool, CODE + layer, rows), tables(layer % 2 == 0)[INVERSE])
            for layer in range(LAYERS)
        ]
        for scen in range(SCEN):
            strip = tree([c[scen][i] * ys[SCEN * i + scen, rows, :] for i in range(3)])
            for layer in range(LAYERS):
                f = scen * LAYERS + layer
                value = c[scen][1] * y1[f, padded, :] + c[scen][2] * y2[f, padded, :] + c[scen][0] * first(f)
                value = jnp.where(edge, turn(strip, 120 - GROUP * layer), value)
                buffer[scen, layer, rows, :] = prev[scen, layer, rows] + scale[layer] * value

    for part in range(parts):
        if part == 0:
            chunk(0, 0, lambda f: y0_fix[f, 0:8, :])
        low = max(1, part * CHUNKS // parts)
        high = min(CHUNKS - 1, (part + 1) * CHUNKS // parts)

        for k in range(low, high):
            chunk(k, 8 * k, lambda f, at=8 * k: y0[f, pl.ds(at + 8, 8), :])

        if part == parts - 1:
            chunk(CHUNKS - 1, TILE - 8, lambda f: y0_fix[f, 8:16, :])
        rows = pl.ds(part * TILE // parts, TILE // parts)
        copy = pltpu.make_async_copy(buffer.at[:, :, rows], out.at[:, :, rows], sems.at[part])
        copy.start()
        copies.append(copy)
    for copy in copies:
        copy.wait()


def swaps(devices):
    near = [(i, i ^ 1) for i in range(devices)]
    far = [(i, i + 1) for i in range(1, devices - 1, 2)]
    return near, far + [(b, a) for a, b in far]


def exchange(a, b, axis):
    near, far = swaps(lax.axis_size(axis))
    return lax.ppermute(a, axis, near), lax.ppermute(b, axis, far)


def coefficients(m):
    h11, h12, h13, h23, h33 = (m[i] - m[i + 1] for i in range(5))
    h22 = h13

    def inverse(x):
        return jnp.where(x > 0, 1.0 / jnp.where(x > 0, x, 1.0), 0.0)

    d1 = inverse(h11)
    l21, l31 = h12 * d1, h13 * d1
    d2 = inverse(h22 - l21 * h12)
    u23 = h23 - l31 * h12
    l32 = u23 * d2
    d3 = inverse(h33 - l31 * h13 - l32 * u23)
    g1 = m[0]
    g2 = m[1] - l21 * g1
    g3 = m[2] - l31 * g1 - l32 * g2
    c3 = g3 * d3
    c2 = g2 * d2 - l32 * c3
    c1 = g1 * d1 - l21 * c2 - l31 * c3
    return c1, c2, c3


def vmem(n):
    return [pl.BlockSpec(memory_space=pltpu.VMEM)] * n


def shape(*dims):
    return jax.ShapeDtypeStruct(dims, F32)


def call(kernel, inputs, outputs, scratch, mib, flops, in_specs=None, out_specs=None):
    many = isinstance(outputs, list)
    return pl.pallas_call(
        kernel,
        in_specs=in_specs or vmem(len(inputs)),
        out_specs=out_specs or (vmem(len(outputs)) if many else vmem(1)[0]),
        out_shape=outputs,
        scratch_shapes=scratch,
        compiler_params=pltpu.CompilerParams(vmem_limit_bytes=int(mib * 2**20)),
        cost_estimate=pl.CostEstimate(flops=flops, bytes_accessed=1 << 20, transcendentals=0),
    )(*inputs)


def per_device(previous, dissipated, material, coolant):
    given = (previous, dissipated, material, coolant)

    def buffer(dtype, *dims):
        return pltpu.VMEM(dims, dtype)

    edges = []
    for a in given:
        edges += [buffer(a.dtype, *a.shape[:-2], 8, TILE)] * 2
    a, b = call(
        pack_rows,
        given,
        [shape(FIELDS * HALO, TILE)] * 2,
        edges + [pltpu.SemaphoreType.DMA((8,))],
        62,
        1 << 20,
        in_specs=[pl.BlockSpec(memory_space=pltpu.HBM)] * 4,
    )
    a, b = exchange(a, b, "gx")
    padded = TILE + 24
    c_blocks, q, y0, m0 = call(
        begin,
        given,
        [shape(5, TILE, TILE), shape(LAYERS, TILE + 8, TILE), shape(PAIRS, padded, TILE), shape(SCEN, 8, TILE)],
        [buffer(F32, LAYERS, padded, TILE), buffer(F32, PAIRS, padded, TILE)],
        8,
        1 << 27,
    )
    a, b, halo, c_halo = call(
        messages,
        (c_blocks, a, b),
        [shape(TILE + 8, TILE)] * 2 + [shape(FIELDS, 8, TILE), shape(5, 8, TILE)],
        [],
        4,
        1 << 20,
    )
    a, b = exchange(a, b, "gy")
    y1, y2, y0_fix, m = call(
        middle,
        (*given, halo, q, y0, m0),
        [shape(PAIRS, padded, TILE)] * 2 + [shape(PAIRS, 16, TILE), shape(SCEN * MOMENTS, 8, TILE)],
        [buffer(F32, LAYERS, 32, TILE)] + [buffer(F32, PAIRS, 32, TILE)] * 4,
        8,
        1 << 27,
    )
    devices = lax.axis_size("gx") * lax.axis_size("gy")
    ys, m = call(
        strips,
        (c_blocks, c_halo, a, b, m),
        [shape(3 * SCEN, TILE, TILE), shape(devices // 8, 8, TILE)],
        [buffer(F32, n, ROWS, TILE) for n in (2, 2, 4, 4, 4, 2, 4, 4, 4)],
        8,
        1 << 24,
    )
    everything = lax.all_to_all(m.reshape(devices, 1, TILE), ("gx", "gy"), split_axis=0, concat_axis=0, tiled=True)
    return call(
        combine,
        (previous, material, coolant, y0, y0_fix, y1, y2, ys, everything.reshape(devices // 8, 8, TILE)),
        shape(*previous.shape),
        [buffer(F32, *previous.shape), pltpu.SemaphoreType.DMA((4,))],
        8,
        1 << 24,
        out_specs=pl.BlockSpec(memory_space=pltpu.HBM),
    )


def solution(mesh):
    placed = (P(None, None, "gx", "gy"),) * 2 + (P(None, "gx", "gy"),) * 2
    return jax.shard_map(
        per_device, mesh=mesh, in_specs=placed, out_specs=P(None, None, "gx", "gy"), check_vma=False
    )
```

```python
import functools

import jax
import jax.numpy as jnp
from jax import lax
from jax.experimental import pallas as pl
from jax.experimental.pallas import tpu as pltpu
from jax.sharding import PartitionSpec as P

TIER_K = (1.0, 0.3, 0.12, 2.5)
CHANNEL_K = (1.0, 0.3, 0.25, 0.2)
CHANNEL_SINK = (0.0, 0.15, 0.45, 1.2)
TIER_HEAT = 0.05
CHANNEL_HEAT = 0.2
VERTICAL = 4.0

SCEN, TIERS, LAYERS = 2, 4, 7
PAIRS = SCEN * LAYERS
TILE = 128
HALO = 4
GROUP = 16
CHUNKS = TILE // 8
FIELDS = PAIRS + SCEN * TIERS + LAYERS
DISS = PAIRS
CODE = DISS + SCEN * TIERS
MOMENTS = 6
F32 = jnp.float32
ROOT, INVERSE, OVER, LOSS = range(4)


def tables(tier):
    if tier:
        kappa, sink, heat = TIER_K, (0.0,) * 4, TIER_HEAT
    else:
        kappa, sink, heat = CHANNEL_K, CHANNEL_SINK, CHANNEL_HEAT
    root = [k**0.5 for k in kappa]
    return (
        (0.0, *root),
        (0.0, *[1.0 / r for r in root]),
        (1.0, *[(heat + s) / r for s, r in zip(sink, root)]),
        (0.0, *[s / r for s, r in zip(sink, root)]),
    )


def pick(code, table):
    out = jnp.full(code.shape, table[0], F32)
    for index in range(1, 5):
        if table[index] != table[0]:
            out = jnp.where(code == float(index), F32(table[index]), out)
    return out


def pick_inside(code, table):
    out = jnp.full(code.shape, table[4], F32)
    for index in range(1, 4):
        if table[index] != table[4]:
            out = jnp.where(code == float(index), F32(table[index]), out)
    return out


def turn(x, shift, axis=1):
    shift %= x.shape[axis]
    return pltpu.roll(x, shift, axis) if shift else x


def tree(terms):
    while len(terms) > 1:
        terms = [terms[i] + terms[i + 1] if i + 1 < len(terms) else terms[i] for i in range(0, len(terms), 2)]
    return terms[0]


def field_rows(previous, dissipated, material, coolant, field, rows):
    if field < DISS:
        return previous[field // LAYERS, field % LAYERS, rows]
    if field < CODE:
        return dissipated[(field - DISS) // TIERS, (field - DISS) % TIERS, rows]
    layer = field - CODE
    block = material[layer // 2, rows] if layer % 2 == 0 else coolant[layer // 2, rows]
    return block.astype(F32) + 1.0


def pack_rows(prev, diss, mat, cool, a_out, b_out, pt, pb, dt, db, mt, mb, ct, cb, sems):
    copies = []
    for index, (source, top, bottom) in enumerate(((prev, pt, pb), (diss, dt, db), (mat, mt, mb), (cool, ct, cb))):
        lead = (slice(None),) * (len(source.shape) - 2)
        for side, (target, at) in enumerate(((top, 0), (bottom, TILE - 8))):
            copies.append(pltpu.make_async_copy(source.at[(*lead, pl.ds(at, 8))], target, sems.at[2 * index + side]))
    for copy in copies:
        copy.start()
    lower = lax.axis_index("gx") % 2 == 0
    for copy in copies:
        copy.wait()
    for field in range(FIELDS):
        top = field_rows(pt, dt, mt, ct, field, slice(0, HALO))
        bottom = field_rows(pb, db, mb, cb, field, slice(8 - HALO, 8))
        rows = slice(HALO * field, HALO * (field + 1))
        a_out[rows, :] = jnp.where(lower, bottom, top)
        b_out[rows, :] = jnp.where(lower, top, bottom)


def strips_of(get, lane):
    zero = jnp.zeros((8, TILE), F32)
    blocks = []
    for fields in (
        [(layer, layer) for layer in range(LAYERS)],
        [(layer, LAYERS + layer) for layer in range(LAYERS)],
        [(layer, CODE + layer) for layer in range(LAYERS)],
        [(2 * t, DISS + t) for t in range(TIERS)],
        [(2 * t, DISS + TIERS + t) for t in range(TIERS)],
    ):
        out = zero
        for layer, field in fields:
            out = jnp.where(lane // GROUP == layer, turn(get(field), GROUP * layer + 8), out)
        blocks.append(out)
    return blocks


def neighbours(ref, base, r, x):
    out = []
    for layer in range(LAYERS):
        f = base + layer
        t = (ref[f, pl.ds(r - 1, 8), :] + ref[f, pl.ds(r + 1, 8), :]) + (turn(x[layer], 1) + turn(x[layer], -1))
        if layer == 0:
            t = t + VERTICAL * x[1]
        elif layer == LAYERS - 1:
            t = t + VERTICAL * x[layer - 1]
        else:
            t = t + VERTICAL * (x[layer - 1] + x[layer + 1])
        out.append(t)
    return out


def rows_of(ref, base, r, count=LAYERS):
    return [ref[base + i, pl.ds(r, 8), :] for i in range(count)]


def start_field(s, code, x, q, ss, syp, base, diss):
    ys, ts = [], []
    for layer in range(LAYERS):
        t = syp[layer] - (pick(code[layer], tables(False)[LOSS]) + ss[layer] if layer % 2 else ss[layer]) * x[layer]
        if layer % 2 == 0:
            t = t + diss[layer // 2] * pick(code[layer], tables(True)[INVERSE])
        ts.append(t)
        ys.append(q[layer] * t)
    return ys, ts


def begin(prev, diss, mat, cool, c_out, q_out, y0_out, m_out, s_ref, yp_ref):
    lane = lax.broadcasted_iota(jnp.int32, (8, TILE), 1)

    for k in range(CHUNKS):
        rows = slice(8 * k, 8 * k + 8)
        inner = slice(8 * k + 8, 8 * k + 16)
        x = [field_rows(prev, diss, mat, cool, f, rows) for f in range(FIELDS)]
        for index, block in enumerate(strips_of(lambda f: x[f], lane)):
            c_out[index, rows, :] = block
        for layer in range(LAYERS):
            s = pick_inside(x[CODE + layer], tables(layer % 2 == 0)[ROOT])
            s_ref[layer, inner, :] = s
            for scen in range(SCEN):
                yp_ref[scen * LAYERS + layer, inner, :] = s * x[scen * LAYERS + layer]

    acc = [jnp.zeros((8, TILE), F32)] * SCEN
    for k in range(CHUNKS):
        rows = slice(8 * k, 8 * k + 8)
        r = 8 * k + 8
        s = rows_of(s_ref, 0, r)
        code = [field_rows(prev, diss, mat, cool, CODE + layer, rows) for layer in range(LAYERS)]
        ss = neighbours(s_ref, 0, r, s)
        q = []
        for layer in range(LAYERS):
            q.append(s[layer] / (pick_inside(code[layer], tables(layer % 2 == 0)[OVER]) + ss[layer]))
            q_out[layer, rows, :] = q[layer]
        sums = []
        for scen in range(SCEN):
            base = scen * LAYERS
            syp = neighbours(yp_ref, base, r, rows_of(yp_ref, base, r))
            x = [prev[scen, layer, rows] for layer in range(LAYERS)]
            d = [diss[scen, t, rows] for t in range(TIERS)]
            y, t = start_field(s, code, x, q, ss, syp, base, d)
            for layer in range(LAYERS):
                y0_out[base + layer, pl.ds(r, 8), :] = y[layer]
            sums.append(tree([a * b for a, b in zip(y, t)]))
        if 0 < k < CHUNKS - 1:
            acc = [a + b for a, b in zip(acc, sums)]
    for scen in range(SCEN):
        m_out[scen] = acc[scen]


def messages(rows_of_devices, c_ref, a_in, b_in, a_out, b_out, halo_out, c_halo):
    lower = lax.axis_index("gx") % 2 == 0
    west = lax.axis_index("gy") % 2 == 0
    at_top, at_bottom = lax.axis_index("gx") == 0, lax.axis_index("gx") == rows_of_devices - 1
    lane = lax.broadcasted_iota(jnp.int32, (8, TILE), 1)
    for field in range(FIELDS):
        rows = slice(HALO * field, HALO * (field + 1))
        a, b = a_in[rows, :], b_in[rows, :]
        above, below = jnp.where(lower, b, a), jnp.where(lower, a, b)
        if field >= CODE:
            above = jnp.where(at_top, 0.0, above)
            below = jnp.where(at_bottom, 0.0, below)
        halo_out[field, :HALO, :] = above
        halo_out[field, HALO:, :] = below
    slot = lane % GROUP // HALO
    odd = lane // GROUP % 2 == 1

    def send(blocks, rows):
        def arrange(base):
            p0, p1, code, d0, d1 = (turn(x, base + HALO * i) for x, i in zip(blocks, (0, 1, 2, 3, 3)))
            d = jnp.where(odd, turn(d1, GROUP), d0)
            return jnp.where(slot < 2, jnp.where(slot == 0, p0, p1), jnp.where(slot == 2, code, d))

        low, high = arrange(-8), arrange(-4)
        a_out[rows, :] = jnp.where(west, high, low)
        b_out[rows, :] = jnp.where(west, low, high)

    for k in range(CHUNKS):
        rows = slice(8 * k, 8 * k + 8)
        send([c_ref[i, rows, :] for i in range(5)], rows)
    blocks = strips_of(lambda f: halo_out[f], lane)
    for index in range(5):
        c_halo[index] = blocks[index]
    send(blocks, slice(TILE, TILE + 8))


def middle(prev, diss, mat, cool, halo, q_ref, y0, m_in, y1, y2, y0_fix, m_out, sn, ypn, y0n, y1n, y2n):
    zero = jnp.zeros((8, TILE), F32)

    def sweep(x_ref, out_ref):
        acc = [zero] * (SCEN if out_ref is None else 2 * SCEN)
        for k in range(CHUNKS):
            if out_ref is None and k in (0, CHUNKS - 1):
                continue
            rows = slice(8 * k, 8 * k + 8)
            r = 8 * k + 8
            odd, even = [], []
            for scen in range(SCEN):
                base = scen * LAYERS
                x = rows_of(x_ref, base, r)
                t = neighbours(x_ref, base, r, x)
                odd.append(tree([a * b for a, b in zip(x, t)]))
                if out_ref is not None:
                    p = []
                    for layer in range(LAYERS):
                        y = q_ref[layer, rows, :] * t[layer]
                        out_ref[base + layer, pl.ds(r, 8), :] = y
                        p.append(y * t[layer])
                    even.append(tree(p))
            if 0 < k < CHUNKS - 1:
                acc = [a + b for a, b in zip(acc, odd + even)]
        return acc

    m = [m_in[scen] for scen in range(SCEN)]
    m += sweep(y0, y1)
    m += sweep(y1, y2)
    m += sweep(y2, None)

    for side in range(2):
        own = 16 if side == 0 else 8
        beyond = 24 - own
        near = slice(0, 8) if side == 0 else slice(TILE - 8, TILE)
        inner = slice(8, 16) if side == 0 else slice(TILE - 16, TILE - 8)
        inner_at = 24 if side == 0 else 0
        chunks = (
            (own, lambda f: field_rows(prev, diss, mat, cool, f, near)),
            (inner_at, lambda f: field_rows(prev, diss, mat, cool, f, inner)),
            (beyond, lambda f: turn(halo[f], 4, 0)),
        )
        for at, get in chunks:
            for layer in range(LAYERS):
                s = pick(get(CODE + layer), tables(layer % 2 == 0)[ROOT])
                sn[layer, at : at + 8, :] = s
                for scen in range(SCEN):
                    ypn[scen * LAYERS + layer, at : at + 8, :] = s * get(scen * LAYERS + layer)
        padded_inner = slice(inner.start + 8, inner.stop + 8)
        padded_near = slice(near.start + 8, near.stop + 8)
        fix = slice(8 * side, 8 * side + 8)
        for f in range(PAIRS):
            y0n[f, inner_at : inner_at + 8, :] = y0[f, padded_inner, :]
            y1n[f, inner_at : inner_at + 8, :] = y1[f, padded_inner, :]
            y2n[f, inner_at : inner_at + 8, :] = y2[f, padded_inner, :]
        q = {}
        for at, get in (chunks[0], chunks[2]):
            s = rows_of(sn, 0, at)
            ss = neighbours(sn, 0, at, s)
            code = [get(CODE + layer) for layer in range(LAYERS)]
            q[at] = [s[i] / (pick(code[i], tables(i % 2 == 0)[OVER]) + ss[i]) for i in range(LAYERS)]
            for scen in range(SCEN):
                base = scen * LAYERS
                syp = neighbours(ypn, base, at, rows_of(ypn, base, at))
                x = [get(base + layer) for layer in range(LAYERS)]
                d = [get(DISS + scen * TIERS + t) for t in range(TIERS)]
                y, t = start_field(s, code, x, q[at], ss, syp, base, d)
                for layer in range(LAYERS):
                    y0n[base + layer, at : at + 8, :] = y[layer]
                    if at == own:
                        y0_fix[base + layer, fix, :] = y[layer]
                if at == own:
                    m[scen] = m[scen] + tree([a * b for a, b in zip(y, t)])
        for level, (x_ref, n_ref, out_ref) in enumerate(((y0n, y1n, y1), (y1n, y2n, y2), (y2n, None, None))):
            for at in (own, beyond) if n_ref is not None else (own,):
                for scen in range(SCEN):
                    base = scen * LAYERS
                    x = rows_of(x_ref, base, at)
                    t = neighbours(x_ref, base, at, x)
                    if at == own:
                        index = SCEN * (2 * level + 1) + scen
                        m[index] = m[index] + tree([a * b for a, b in zip(x, t)])
                    if n_ref is None:
                        continue
                    p = []
                    for layer in range(LAYERS):
                        y = q[at][layer] * t[layer]
                        n_ref[base + layer, at : at + 8, :] = y
                        if at == own:
                            out_ref[base + layer, padded_near, :] = y
                            p.append(y * t[layer])
                    if at == own:
                        index = SCEN * (2 * level + 2) + scen
                        m[index] = m[index] + tree(p)
    for index in range(SCEN * MOMENTS):
        m_out[index] = m[index]


TOP = 16
ROWS = TOP + TILE + 16


def strips(columns_of_devices, c_ref, c_halo, a_in, b_in, m_in, ys_out, m_out, code_ref, s_ref, x_ref, d_ref, yp_ref, q_ref, y0, y1, y2):
    west = lax.axis_index("gy") % 2 == 0
    lane = lax.broadcasted_iota(jnp.int32, (8, TILE), 1)
    outside = [lax.axis_index("gy") == end for end in (columns_of_devices - 1, 0)]
    place = lane % GROUP
    real = lane < GROUP * LAYERS
    tier = lane // GROUP % 2 == 0
    zero = jnp.zeros((8, TILE), F32)
    sides = (
        (place < 8, (place >= 8) & (place < 12) & real, (place >= 4) & (place < 8) & real, 8),
        (place >= 8, (place >= 4) & (place < 8) & real, (place >= 8) & (place < 12) & real, 4),
    )

    def lookup(code, kind):
        out = zero if tables(True)[kind][0] == 0.0 else jnp.full_like(zero, tables(True)[kind][0])
        for index in range(1, 5):
            value = jnp.where(tier, F32(tables(True)[kind][index]), F32(tables(False)[kind][index]))
            out = jnp.where(code == float(index), value, out)
        return out

    chunk_rows = [(slice(8 * k, 8 * k + 8), (8 * k + TOP,), 0) for k in range(CHUNKS)]
    chunk_rows.append((None, (TOP - 8, TOP + TILE), 4))
    for rows, targets, rotation in chunk_rows:
        message = slice(TILE, TILE + 8) if rows is None else rows
        a, b = a_in[message, :], b_in[message, :]
        blocks = [c_halo[i] if rows is None else c_ref[i, rows, :] for i in range(5)]
        for side, (own, beyond, _, base) in enumerate(sides):
            got = jnp.where(west, a, b) if side == 0 else jnp.where(west, b, a)
            got = jnp.where(outside[side], 0.0, got)
            full = []
            for index, shift in enumerate((base, base - 4, base - 8, base - 12, base - 12 - GROUP)):
                mask = beyond if index < 3 else beyond & tier
                full.append(jnp.where(own, blocks[index], jnp.where(mask, turn(got, shift), zero)))
            full = [turn(x, rotation, 0) for x in full]
            s = lookup(full[2], ROOT)
            for at in targets:
                here = slice(at, at + 8)
                code_ref[side, here, :] = full[2]
                s_ref[side, here, :] = s
                for scen in range(SCEN):
                    x_ref[2 * scen + side, here, :] = full[scen]
                    d_ref[2 * scen + side, here, :] = full[3 + scen]
                    yp_ref[2 * scen + side, here, :] = s * full[scen]

    def around(ref, index, at):
        x = ref[index, at : at + 8, :]
        lateral = (ref[index, at - 1 : at + 7, :] + ref[index, at + 1 : at + 9, :]) + (turn(x, 1) + turn(x, -1))
        return x, lateral + VERTICAL * (turn(x, GROUP) + turn(x, -GROUP))

    everywhere = range(TOP - 8, TOP + TILE + 8, 8)
    within = range(TOP, TOP + TILE, 8)
    m = [[zero, zero] for _ in range(SCEN * MOMENTS)]

    def count(index, side, at, value):
        if at in within:
            m[index][side] = m[index][side] + value

    for at in everywhere:
        here = slice(at, at + 8)
        for side in range(2):
            code = code_ref[side, here, :]
            s, ss = around(s_ref, side, at)
            q = s / (lookup(code, OVER) + ss)
            q_ref[side, here, :] = q
            inverse, loss = lookup(code, INVERSE), lookup(code, LOSS) + ss
            for scen in range(SCEN):
                f = 2 * scen + side
                _, syp = around(yp_ref, f, at)
                t = syp - loss * x_ref[f, here, :] + d_ref[f, here, :] * inverse
                y = q * t
                y0[f, here, :] = y
                count(scen, side, at, y * t)
    for level, (ref, out) in enumerate(((y0, y1), (y1, y2), (y2, None))):
        for at in everywhere if out is not None else within:
            here = slice(at, at + 8)
            for side in range(2):
                for scen in range(SCEN):
                    f = 2 * scen + side
                    x, t = around(ref, f, at)
                    count(SCEN * (2 * level + 1) + scen, side, at, x * t)
                    if out is not None:
                        y = q_ref[side, here, :] * t
                        out[f, here, :] = y
                        count(SCEN * (2 * level + 2) + scen, side, at, y * t)
    for level, ref in enumerate((y0, y1, y2)):
        for scen in range(SCEN):
            for k in range(CHUNKS):
                here = slice(8 * k + TOP, 8 * k + TOP + 8)
                merged = jnp.where(place < 8, ref[2 * scen, here, :], ref[2 * scen + 1, here, :])
                ys_out[SCEN * level + scen, 8 * k : 8 * k + 8, :] = merged
    line = lax.broadcasted_iota(jnp.int32, (8, TILE), 1)
    inner = (lane >= HALO) & (lane < TILE - HALO)
    out = zero
    for index in range(SCEN * MOMENTS):
        east, wst = (jnp.where(sides[side][2], m[index][side], 0.0) for side in range(2))
        value = jnp.where(inner, m_in[index], 0.0) + (east + wst)
        value = jnp.sum(jnp.sum(value, axis=0, keepdims=True), axis=1, keepdims=True)
        out = jnp.where(line == index, value, out)
    m_out[...] = jnp.broadcast_to(out, m_out.shape)


def combine(prev, mat, cool, y0, y0_fix, y1, y2, ys, m_ref, out, buffer, sems):
    lane = lax.broadcasted_iota(jnp.int32, (8, TILE), 1)
    edge = (lane < HALO) | (lane >= TILE - HALO)
    total = tree([m_ref[i] for i in range(m_ref.shape[0])])
    total = jnp.broadcast_to(jnp.sum(total, axis=0, keepdims=True), (8, TILE))
    weights = coefficients([turn(total, -SCEN * i) for i in range(MOMENTS)])
    c = [
        [jnp.broadcast_to(jnp.sum(jnp.where(lane == scen, w, 0.0), axis=1, keepdims=True), (8, TILE)) for w in weights]
        for scen in range(SCEN)
    ]
    parts = 4
    copies = []

    def chunk(k, at, first):
        rows = pl.ds(at, 8)
        padded = pl.ds(at + 8, 8)
        scale = [
            pick_inside(field_rows(prev, None, mat, cool, CODE + layer, rows), tables(layer % 2 == 0)[INVERSE])
            for layer in range(LAYERS)
        ]
        for scen in range(SCEN):
            strip = tree([c[scen][i] * ys[SCEN * i + scen, rows, :] for i in range(3)])
            for layer in range(LAYERS):
                f = scen * LAYERS + layer
                value = c[scen][1] * y1[f, padded, :] + c[scen][2] * y2[f, padded, :] + c[scen][0] * first(f)
                value = jnp.where(edge, turn(strip, 120 - GROUP * layer), value)
                buffer[scen, layer, rows, :] = prev[scen, layer, rows] + scale[layer] * value

    for part in range(parts):
        if part == 0:
            chunk(0, 0, lambda f: y0_fix[f, 0:8, :])
        low = max(1, part * CHUNKS // parts)
        high = min(CHUNKS - 1, (part + 1) * CHUNKS // parts)

        for k in range(low, high):
            chunk(k, 8 * k, lambda f, at=8 * k: y0[f, pl.ds(at + 8, 8), :])

        if part == parts - 1:
            chunk(CHUNKS - 1, TILE - 8, lambda f: y0_fix[f, 8:16, :])
        rows = pl.ds(part * TILE // parts, TILE // parts)
        copy = pltpu.make_async_copy(buffer.at[:, :, rows], out.at[:, :, rows], sems.at[part])
        copy.start()
        copies.append(copy)
    for copy in copies:
        copy.wait()


def swaps(devices):
    near = [(i, i ^ 1) for i in range(devices)]
    far = [(i, (i + 1) % devices) for i in range(1, devices, 2)]
    return near, far + [(b, a) for a, b in far]


def exchange(a, b, axis):
    near, far = swaps(lax.axis_size(axis))
    return lax.ppermute(a, axis, near), lax.ppermute(b, axis, far)


def coefficients(m):
    h11, h12, h13, h23, h33 = (m[i] - m[i + 1] for i in range(5))
    h22 = h13

    def inverse(x):
        return jnp.where(x > 0, 1.0 / jnp.where(x > 0, x, 1.0), 0.0)

    d1 = inverse(h11)
    l21, l31 = h12 * d1, h13 * d1
    d2 = inverse(h22 - l21 * h12)
    u23 = h23 - l31 * h12
    l32 = u23 * d2
    d3 = inverse(h33 - l31 * h13 - l32 * u23)
    g1 = m[0]
    g2 = m[1] - l21 * g1
    g3 = m[2] - l31 * g1 - l32 * g2
    c3 = g3 * d3
    c2 = g2 * d2 - l32 * c3
    c1 = g1 * d1 - l21 * c2 - l31 * c3
    return c1, c2, c3


def vmem(n):
    return [pl.BlockSpec(memory_space=pltpu.VMEM)] * n


def shape(*dims):
    return jax.ShapeDtypeStruct(dims, F32)


def call(kernel, inputs, outputs, scratch, mib, flops, in_specs=None, out_specs=None):
    many = isinstance(outputs, list)
    return pl.pallas_call(
        kernel,
        in_specs=in_specs or vmem(len(inputs)),
        out_specs=out_specs or (vmem(len(outputs)) if many else vmem(1)[0]),
        out_shape=outputs,
        scratch_shapes=scratch,
        compiler_params=pltpu.CompilerParams(vmem_limit_bytes=int(mib * 2**20)),
        cost_estimate=pl.CostEstimate(flops=flops, bytes_accessed=1 << 20, transcendentals=0),
    )(*inputs)


def per_device(previous, dissipated, material, coolant):
    given = (previous, dissipated, material, coolant)

    def buffer(dtype, *dims):
        return pltpu.VMEM(dims, dtype)

    edges = []
    for a in given:
        edges += [buffer(a.dtype, *a.shape[:-2], 8, TILE)] * 2
    a, b = call(
        pack_rows,
        [pltpu.with_memory_space_constraint(x, pltpu.HBM) for x in given],
        [pltpu.VMEM((FIELDS * HALO, TILE), F32)] * 2,
        edges + [pltpu.SemaphoreType.DMA((8,))],
        4,
        1 << 20,
        in_specs=[pl.BlockSpec(memory_space=pltpu.HBM)] * 4,
    )
    a, b = exchange(a, b, "gx")
    padded = TILE + 24
    c_blocks, q, y0, m0 = call(
        begin,
        given,
        [shape(5, TILE, TILE), shape(LAYERS, TILE + 8, TILE), shape(PAIRS, padded, TILE), shape(SCEN, 8, TILE)],
        [buffer(F32, LAYERS, padded, TILE), buffer(F32, PAIRS, padded, TILE)],
        8,
        1 << 27,
    )
    a, b, halo, c_halo = call(
        functools.partial(messages, lax.axis_size("gx")),
        (c_blocks, a, b),
        [shape(TILE + 8, TILE)] * 2 + [shape(FIELDS, 8, TILE), shape(5, 8, TILE)],
        [],
        4,
        1 << 20,
    )
    a, b = exchange(a, b, "gy")
    y1, y2, y0_fix, m = call(
        middle,
        (*given, halo, q, y0, m0),
        [shape(PAIRS, padded, TILE)] * 2 + [shape(PAIRS, 16, TILE), shape(SCEN * MOMENTS, 8, TILE)],
        [buffer(F32, LAYERS, 32, TILE)] + [buffer(F32, PAIRS, 32, TILE)] * 4,
        8,
        1 << 27,
    )
    devices = lax.axis_size("gx") * lax.axis_size("gy")
    ys, m = call(
        functools.partial(strips, lax.axis_size("gy")),
        (c_blocks, c_halo, a, b, m),
        [shape(3 * SCEN, TILE, TILE), shape(devices // 8, 8, TILE)],
        [buffer(F32, n, ROWS, TILE) for n in (2, 2, 4, 4, 4, 2, 4, 4, 4)],
        8,
        1 << 24,
    )
    everything = lax.all_to_all(m.reshape(devices, 1, TILE), ("gx", "gy"), split_axis=0, concat_axis=0, tiled=True)
    return call(
        combine,
        (previous, material, coolant, y0, y0_fix, y1, y2, ys, everything.reshape(devices // 8, 8, TILE)),
        shape(*previous.shape),
        [buffer(F32, *previous.shape), pltpu.SemaphoreType.DMA((4,))],
        8,
        1 << 24,
        out_specs=pl.BlockSpec(memory_space=pltpu.HBM),
    )


def solution(mesh):
    placed = (P(None, None, "gx", "gy"),) * 2 + (P(None, "gx", "gy"),) * 2
    return jax.shard_map(
        per_device, mesh=mesh, in_specs=placed, out_specs=P(None, None, "gx", "gy"), check_vma=False
    )
```

```python
import functools

import jax
import jax.numpy as jnp
from jax import lax
from jax.experimental import pallas as pl
from jax.experimental.pallas import tpu as pltpu
from jax.sharding import PartitionSpec as P

TIER_K = (1.0, 0.3, 0.12, 2.5)
CHANNEL_K = (1.0, 0.3, 0.25, 0.2)
CHANNEL_SINK = (0.0, 0.15, 0.45, 1.2)
TIER_HEAT = 0.05
CHANNEL_HEAT = 0.2
VERTICAL = 4.0

SCEN, TIERS, LAYERS = 2, 4, 7
PAIRS = SCEN * LAYERS
TILE = 128
HALO = 4
GROUP = 16
CHUNKS = TILE // 8
FIELDS = PAIRS + SCEN * TIERS + LAYERS
DISS = PAIRS
CODE = DISS + SCEN * TIERS
MOMENTS = 6
F32 = jnp.float32
ROOT, INVERSE, OVER, LOSS = range(4)


def tables(tier):
    if tier:
        kappa, sink, heat = TIER_K, (0.0,) * 4, TIER_HEAT
    else:
        kappa, sink, heat = CHANNEL_K, CHANNEL_SINK, CHANNEL_HEAT
    root = [k**0.5 for k in kappa]
    return (
        (0.0, *root),
        (0.0, *[1.0 / r for r in root]),
        (1.0, *[(heat + s) / r for s, r in zip(sink, root)]),
        (0.0, *[s / r for s, r in zip(sink, root)]),
    )


def pick(code, table):
    out = jnp.full(code.shape, table[0], F32)
    for index in range(1, 5):
        if table[index] != table[0]:
            out = jnp.where(code == float(index), F32(table[index]), out)
    return out


def pick_inside(code, table):
    out = jnp.full(code.shape, table[4], F32)
    for index in range(1, 4):
        if table[index] != table[4]:
            out = jnp.where(code == float(index), F32(table[index]), out)
    return out


def turn(x, shift, axis=1):
    shift %= x.shape[axis]
    return pltpu.roll(x, shift, axis) if shift else x


def tree(terms):
    while len(terms) > 1:
        terms = [terms[i] + terms[i + 1] if i + 1 < len(terms) else terms[i] for i in range(0, len(terms), 2)]
    return terms[0]


def field_rows(previous, dissipated, material, coolant, field, rows):
    if field < DISS:
        return previous[field // LAYERS, field % LAYERS, rows]
    if field < CODE:
        return dissipated[(field - DISS) // TIERS, (field - DISS) % TIERS, rows]
    layer = field - CODE
    block = material[layer // 2, rows] if layer % 2 == 0 else coolant[layer // 2, rows]
    return block.astype(F32) + 1.0


def pack_rows(prev, diss, mat, cool, a_out, b_out, pt, pb, dt, db, mt, mb, ct, cb, sems):
    copies = []
    for index, (source, top, bottom) in enumerate(((prev, pt, pb), (diss, dt, db), (mat, mt, mb), (cool, ct, cb))):
        lead = (slice(None),) * (len(source.shape) - 2)
        for side, (target, at) in enumerate(((top, 0), (bottom, TILE - 8))):
            copies.append(pltpu.make_async_copy(source.at[(*lead, pl.ds(at, 8))], target, sems.at[2 * index + side]))
    for copy in copies:
        copy.start()
    lower = lax.axis_index("gx") % 2 == 0
    for copy in copies:
        copy.wait()
    for field in range(FIELDS):
        top = field_rows(pt, dt, mt, ct, field, slice(0, HALO))
        bottom = field_rows(pb, db, mb, cb, field, slice(8 - HALO, 8))
        rows = slice(HALO * field, HALO * (field + 1))
        a_out[rows, :] = jnp.where(lower, bottom, top)
        b_out[rows, :] = jnp.where(lower, top, bottom)


def strips_of(get, lane):
    zero = jnp.zeros((8, TILE), F32)
    blocks = []
    for fields in (
        [(layer, layer) for layer in range(LAYERS)],
        [(layer, LAYERS + layer) for layer in range(LAYERS)],
        [(layer, CODE + layer) for layer in range(LAYERS)],
        [(2 * t + scen, DISS + TIERS * scen + t) for t in range(TIERS) for scen in range(SCEN)],
    ):
        out = zero
        for layer, field in fields:
            out = jnp.where(lane // GROUP == layer, turn(get(field), GROUP * layer + 8), out)
        blocks.append(out)
    return blocks


def neighbours(ref, base, r, x):
    out = []
    for layer in range(LAYERS):
        f = base + layer
        t = (ref[f, pl.ds(r - 1, 8), :] + ref[f, pl.ds(r + 1, 8), :]) + (turn(x[layer], 1) + turn(x[layer], -1))
        if layer == 0:
            t = t + VERTICAL * x[1]
        elif layer == LAYERS - 1:
            t = t + VERTICAL * x[layer - 1]
        else:
            t = t + VERTICAL * (x[layer - 1] + x[layer + 1])
        out.append(t)
    return out


def rows_of(ref, base, r, count=LAYERS):
    return [ref[base + i, pl.ds(r, 8), :] for i in range(count)]


def start_field(s, code, x, q, ss, syp, base, diss):
    ys, ts = [], []
    for layer in range(LAYERS):
        t = syp[layer] - (pick(code[layer], tables(False)[LOSS]) + ss[layer] if layer % 2 else ss[layer]) * x[layer]
        if layer % 2 == 0:
            t = t + diss[layer // 2] * pick(code[layer], tables(True)[INVERSE])
        ts.append(t)
        ys.append(q[layer] * t)
    return ys, ts


def begin(prev, diss, mat, cool, c_out, q_out, y0_out, m_out, s_ref, yp_ref):
    lane = lax.broadcasted_iota(jnp.int32, (8, TILE), 1)

    for k in range(CHUNKS):
        rows = slice(8 * k, 8 * k + 8)
        inner = slice(8 * k + 8, 8 * k + 16)
        x = [field_rows(prev, diss, mat, cool, f, rows) for f in range(FIELDS)]
        for index, block in enumerate(strips_of(lambda f: x[f], lane)):
            c_out[index, rows, :] = block
        for layer in range(LAYERS):
            s = pick_inside(x[CODE + layer], tables(layer % 2 == 0)[ROOT])
            s_ref[layer, inner, :] = s
            for scen in range(SCEN):
                yp_ref[scen * LAYERS + layer, inner, :] = s * x[scen * LAYERS + layer]

    acc = [jnp.zeros((8, TILE), F32)] * SCEN
    for k in range(CHUNKS):
        rows = slice(8 * k, 8 * k + 8)
        r = 8 * k + 8
        s = rows_of(s_ref, 0, r)
        code = [field_rows(prev, diss, mat, cool, CODE + layer, rows) for layer in range(LAYERS)]
        ss = neighbours(s_ref, 0, r, s)
        q = []
        for layer in range(LAYERS):
            q.append(s[layer] / (pick_inside(code[layer], tables(layer % 2 == 0)[OVER]) + ss[layer]))
            q_out[layer, rows, :] = q[layer]
        sums = []
        for scen in range(SCEN):
            base = scen * LAYERS
            syp = neighbours(yp_ref, base, r, rows_of(yp_ref, base, r))
            x = [prev[scen, layer, rows] for layer in range(LAYERS)]
            d = [diss[scen, t, rows] for t in range(TIERS)]
            y, t = start_field(s, code, x, q, ss, syp, base, d)
            for layer in range(LAYERS):
                y0_out[base + layer, pl.ds(r, 8), :] = y[layer]
            sums.append(tree([a * b for a, b in zip(y, t)]))
        if 0 < k < CHUNKS - 1:
            acc = [a + b for a, b in zip(acc, sums)]
    for scen in range(SCEN):
        m_out[scen] = acc[scen]


def messages(rows_of_devices, c_ref, a_in, b_in, a_out, b_out, halo_out, c_halo):
    lower = lax.axis_index("gx") % 2 == 0
    west = lax.axis_index("gy") % 2 == 0
    at_top, at_bottom = lax.axis_index("gx") == 0, lax.axis_index("gx") == rows_of_devices - 1
    lane = lax.broadcasted_iota(jnp.int32, (8, TILE), 1)
    for field in range(FIELDS):
        rows = slice(HALO * field, HALO * (field + 1))
        a, b = a_in[rows, :], b_in[rows, :]
        above, below = jnp.where(lower, b, a), jnp.where(lower, a, b)
        if field >= CODE:
            above = jnp.where(at_top, 0.0, above)
            below = jnp.where(at_bottom, 0.0, below)
        halo_out[field, :HALO, :] = above
        halo_out[field, HALO:, :] = below
    slot = lane % GROUP // HALO

    def send(blocks, rows):
        p0, p1, code, d = (turn(x, HALO * i - 8) for i, x in enumerate(blocks))

        def by_slot(a, b, c, e):
            return jnp.where(slot < 2, jnp.where(slot == 0, a, b), jnp.where(slot == 2, c, e))

        low, high = by_slot(p0, p1, code, d), by_slot(p1, code, d, p0)
        a_out[rows, :] = jnp.where(west, high, low)
        b_out[rows, :] = jnp.where(west, low, high)

    for k in range(CHUNKS):
        rows = slice(8 * k, 8 * k + 8)
        send([c_ref[i, rows, :] for i in range(4)], rows)
    blocks = strips_of(lambda f: halo_out[f], lane)
    for index in range(4):
        c_halo[index] = blocks[index]
    send(blocks, slice(TILE, TILE + 8))


def middle(prev, diss, mat, cool, halo, q_ref, y0, m_in, y1, y2, y0_fix, m_out, sn, ypn, y0n, y1n, y2n):
    zero = jnp.zeros((8, TILE), F32)

    def sweep(x_ref, out_ref):
        acc = [zero] * (SCEN if out_ref is None else 2 * SCEN)
        for k in range(CHUNKS):
            if out_ref is None and k in (0, CHUNKS - 1):
                continue
            rows = slice(8 * k, 8 * k + 8)
            r = 8 * k + 8
            odd, even = [], []
            for scen in range(SCEN):
                base = scen * LAYERS
                x = rows_of(x_ref, base, r)
                t = neighbours(x_ref, base, r, x)
                odd.append(tree([a * b for a, b in zip(x, t)]))
                if out_ref is not None:
                    p = []
                    for layer in range(LAYERS):
                        y = q_ref[layer, rows, :] * t[layer]
                        out_ref[base + layer, pl.ds(r, 8), :] = y
                        p.append(y * t[layer])
                    even.append(tree(p))
            if 0 < k < CHUNKS - 1:
                acc = [a + b for a, b in zip(acc, odd + even)]
        return acc

    m = [m_in[scen] for scen in range(SCEN)]
    m += sweep(y0, y1)
    m += sweep(y1, y2)
    m += sweep(y2, None)

    for side in range(2):
        own = 16 if side == 0 else 8
        beyond = 24 - own
        near = slice(0, 8) if side == 0 else slice(TILE - 8, TILE)
        inner = slice(8, 16) if side == 0 else slice(TILE - 16, TILE - 8)
        inner_at = 24 if side == 0 else 0
        chunks = (
            (own, lambda f: field_rows(prev, diss, mat, cool, f, near)),
            (inner_at, lambda f: field_rows(prev, diss, mat, cool, f, inner)),
            (beyond, lambda f: turn(halo[f], 4, 0)),
        )
        for at, get in chunks:
            for layer in range(LAYERS):
                s = pick(get(CODE + layer), tables(layer % 2 == 0)[ROOT])
                sn[layer, at : at + 8, :] = s
                for scen in range(SCEN):
                    ypn[scen * LAYERS + layer, at : at + 8, :] = s * get(scen * LAYERS + layer)
        padded_inner = slice(inner.start + 8, inner.stop + 8)
        padded_near = slice(near.start + 8, near.stop + 8)
        fix = slice(8 * side, 8 * side + 8)
        for f in range(PAIRS):
            y0n[f, inner_at : inner_at + 8, :] = y0[f, padded_inner, :]
            y1n[f, inner_at : inner_at + 8, :] = y1[f, padded_inner, :]
            y2n[f, inner_at : inner_at + 8, :] = y2[f, padded_inner, :]
        q = {}
        for at, get in (chunks[0], chunks[2]):
            s = rows_of(sn, 0, at)
            ss = neighbours(sn, 0, at, s)
            code = [get(CODE + layer) for layer in range(LAYERS)]
            q[at] = [s[i] / (pick(code[i], tables(i % 2 == 0)[OVER]) + ss[i]) for i in range(LAYERS)]
            for scen in range(SCEN):
                base = scen * LAYERS
                syp = neighbours(ypn, base, at, rows_of(ypn, base, at))
                x = [get(base + layer) for layer in range(LAYERS)]
                d = [get(DISS + scen * TIERS + t) for t in range(TIERS)]
                y, t = start_field(s, code, x, q[at], ss, syp, base, d)
                for layer in range(LAYERS):
                    y0n[base + layer, at : at + 8, :] = y[layer]
                    if at == own:
                        y0_fix[base + layer, fix, :] = y[layer]
                if at == own:
                    m[scen] = m[scen] + tree([a * b for a, b in zip(y, t)])
        for level, (x_ref, n_ref, out_ref) in enumerate(((y0n, y1n, y1), (y1n, y2n, y2), (y2n, None, None))):
            for at in (own, beyond) if n_ref is not None else (own,):
                for scen in range(SCEN):
                    base = scen * LAYERS
                    x = rows_of(x_ref, base, at)
                    t = neighbours(x_ref, base, at, x)
                    if at == own:
                        index = SCEN * (2 * level + 1) + scen
                        m[index] = m[index] + tree([a * b for a, b in zip(x, t)])
                    if n_ref is None:
                        continue
                    p = []
                    for layer in range(LAYERS):
                        y = q[at][layer] * t[layer]
                        n_ref[base + layer, at : at + 8, :] = y
                        if at == own:
                            out_ref[base + layer, padded_near, :] = y
                            p.append(y * t[layer])
                    if at == own:
                        index = SCEN * (2 * level + 2) + scen
                        m[index] = m[index] + tree(p)
    for index in range(SCEN * MOMENTS):
        m_out[index] = m[index]


TOP = 16
ROWS = TOP + TILE + 16


def strips(columns_of_devices, c_ref, c_halo, a_in, b_in, m_in, ys_out, m_out, code_ref, s_ref, x_ref, d_ref, yp_ref, q_ref, y0, y1, y2):
    west = lax.axis_index("gy") % 2 == 0
    lane = lax.broadcasted_iota(jnp.int32, (8, TILE), 1)
    outside = [lax.axis_index("gy") == end for end in (columns_of_devices - 1, 0)]
    place = lane % GROUP
    real = lane < GROUP * LAYERS
    tier = lane // GROUP % 2 == 0
    zero = jnp.zeros((8, TILE), F32)
    slot = place // HALO
    sides = (
        (place < 8, (place >= 8) & (place < 12), (place >= 4) & (place < 8) & real),
        (place >= 8, (place >= 4) & (place < 8), (place >= 8) & (place < 12) & real),
    )

    def lookup(code, kind):
        out = zero if tables(True)[kind][0] == 0.0 else jnp.full_like(zero, tables(True)[kind][0])
        for index in range(1, 5):
            value = jnp.where(tier, F32(tables(True)[kind][index]), F32(tables(False)[kind][index]))
            out = jnp.where(code == float(index), value, out)
        return out

    chunk_rows = [(slice(8 * k, 8 * k + 8), (8 * k + TOP,), 0) for k in range(CHUNKS)]
    chunk_rows.append((None, (TOP - 8, TOP + TILE), 4))
    for rows, targets, rotation in chunk_rows:
        message = slice(TILE, TILE + 8) if rows is None else rows
        a, b = a_in[message, :], b_in[message, :]
        blocks = [c_halo[i] if rows is None else c_ref[i, rows, :] for i in range(4)]
        east = jnp.where(outside[0], 0.0, jnp.where(west, a, b))
        wst = jnp.where(outside[1], 0.0, jnp.where(west, b, a))
        got = [turn(jnp.where(slot == i, east, wst), 8 - HALO * i) for i in range(4)]
        for side, (own, beyond, _) in enumerate(sides):
            full = [jnp.where(own, x, jnp.where(beyond, y, zero)) for x, y in zip(blocks, got)]
            full[2] = jnp.where(real, full[2], zero)
            full[3:] = [jnp.where(tier, full[3], zero), jnp.where(tier, turn(full[3], -GROUP), zero)]
            full = [turn(x, rotation, 0) for x in full]
            s = lookup(full[2], ROOT)
            for at in targets:
                here = slice(at, at + 8)
                code_ref[side, here, :] = full[2]
                s_ref[side, here, :] = s
                for scen in range(SCEN):
                    x_ref[2 * scen + side, here, :] = full[scen]
                    d_ref[2 * scen + side, here, :] = full[3 + scen]
                    yp_ref[2 * scen + side, here, :] = s * full[scen]

    def around(ref, index, at):
        x = ref[index, at : at + 8, :]
        lateral = (ref[index, at - 1 : at + 7, :] + ref[index, at + 1 : at + 9, :]) + (turn(x, 1) + turn(x, -1))
        return x, lateral + VERTICAL * (turn(x, GROUP) + turn(x, -GROUP))

    everywhere = range(TOP - 8, TOP + TILE + 8, 8)
    within = range(TOP, TOP + TILE, 8)
    m = [[zero, zero] for _ in range(SCEN * MOMENTS)]

    def count(index, side, at, value):
        if at in within:
            m[index][side] = m[index][side] + value

    for at in everywhere:
        here = slice(at, at + 8)
        for side in range(2):
            code = code_ref[side, here, :]
            s, ss = around(s_ref, side, at)
            q = s / (lookup(code, OVER) + ss)
            q_ref[side, here, :] = q
            inverse, loss = lookup(code, INVERSE), lookup(code, LOSS) + ss
            for scen in range(SCEN):
                f = 2 * scen + side
                _, syp = around(yp_ref, f, at)
                t = syp - loss * x_ref[f, here, :] + d_ref[f, here, :] * inverse
                y = q * t
                y0[f, here, :] = y
                count(scen, side, at, y * t)
    for level, (ref, out) in enumerate(((y0, y1), (y1, y2), (y2, None))):
        for at in everywhere if out is not None else within:
            here = slice(at, at + 8)
            for side in range(2):
                for scen in range(SCEN):
                    f = 2 * scen + side
                    x, t = around(ref, f, at)
                    count(SCEN * (2 * level + 1) + scen, side, at, x * t)
                    if out is not None:
                        y = q_ref[side, here, :] * t
                        out[f, here, :] = y
                        count(SCEN * (2 * level + 2) + scen, side, at, y * t)
    for level, ref in enumerate((y0, y1, y2)):
        for scen in range(SCEN):
            for k in range(CHUNKS):
                here = slice(8 * k + TOP, 8 * k + TOP + 8)
                merged = jnp.where(place < 8, ref[2 * scen, here, :], ref[2 * scen + 1, here, :])
                ys_out[SCEN * level + scen, 8 * k : 8 * k + 8, :] = merged
    line = lax.broadcasted_iota(jnp.int32, (8, TILE), 1)
    inner = (lane >= HALO) & (lane < TILE - HALO)
    out = zero
    for index in range(SCEN * MOMENTS):
        east, wst = (jnp.where(sides[side][2], m[index][side], 0.0) for side in range(2))
        value = jnp.where(inner, m_in[index], 0.0) + (east + wst)
        value = jnp.sum(jnp.sum(value, axis=0, keepdims=True), axis=1, keepdims=True)
        out = jnp.where(line == index, value, out)
    m_out[...] = jnp.broadcast_to(out, m_out.shape)


def combine(prev, mat, cool, y0, y0_fix, y1, y2, ys, m_ref, out, buffer, sems):
    lane = lax.broadcasted_iota(jnp.int32, (8, TILE), 1)
    edge = (lane < HALO) | (lane >= TILE - HALO)
    total = tree([m_ref[i] for i in range(m_ref.shape[0])])
    total = jnp.broadcast_to(jnp.sum(total, axis=0, keepdims=True), (8, TILE))
    weights = coefficients([turn(total, -SCEN * i) for i in range(MOMENTS)])
    c = [
        [jnp.broadcast_to(jnp.sum(jnp.where(lane == scen, w, 0.0), axis=1, keepdims=True), (8, TILE)) for w in weights]
        for scen in range(SCEN)
    ]
    parts = 4
    copies = []

    def chunk(k, at, first):
        rows = pl.ds(at, 8)
        padded = pl.ds(at + 8, 8)
        scale = [
            pick_inside(field_rows(prev, None, mat, cool, CODE + layer, rows), tables(layer % 2 == 0)[INVERSE])
            for layer in range(LAYERS)
        ]
        for scen in range(SCEN):
            strip = tree([c[scen][i] * ys[SCEN * i + scen, rows, :] for i in range(3)])
            for layer in range(LAYERS):
                f = scen * LAYERS + layer
                value = c[scen][1] * y1[f, padded, :] + c[scen][2] * y2[f, padded, :] + c[scen][0] * first(f)
                value = jnp.where(edge, turn(strip, 120 - GROUP * layer), value)
                buffer[scen, layer, rows, :] = prev[scen, layer, rows] + scale[layer] * value

    for part in range(parts):
        if part == 0:
            chunk(0, 0, lambda f: y0_fix[f, 0:8, :])
        low = max(1, part * CHUNKS // parts)
        high = min(CHUNKS - 1, (part + 1) * CHUNKS // parts)

        for k in range(low, high):
            chunk(k, 8 * k, lambda f, at=8 * k: y0[f, pl.ds(at + 8, 8), :])

        if part == parts - 1:
            chunk(CHUNKS - 1, TILE - 8, lambda f: y0_fix[f, 8:16, :])
        rows = pl.ds(part * TILE // parts, TILE // parts)
        copy = pltpu.make_async_copy(buffer.at[:, :, rows], out.at[:, :, rows], sems.at[part])
        copy.start()
        copies.append(copy)
    for copy in copies:
        copy.wait()


def swaps(devices):
    near = [(i, i ^ 1) for i in range(devices)]
    far = [(i, (i + 1) % devices) for i in range(1, devices, 2)]
    return near, far + [(b, a) for a, b in far]


def exchange(a, b, axis):
    near, far = swaps(lax.axis_size(axis))
    return lax.ppermute(a, axis, near), lax.ppermute(b, axis, far)


def coefficients(m):
    h11, h12, h13, h23, h33 = (m[i] - m[i + 1] for i in range(5))
    h22 = h13

    def inverse(x):
        return jnp.where(x > 0, 1.0 / jnp.where(x > 0, x, 1.0), 0.0)

    d1 = inverse(h11)
    l21, l31 = h12 * d1, h13 * d1
    d2 = inverse(h22 - l21 * h12)
    u23 = h23 - l31 * h12
    l32 = u23 * d2
    d3 = inverse(h33 - l31 * h13 - l32 * u23)
    g1 = m[0]
    g2 = m[1] - l21 * g1
    g3 = m[2] - l31 * g1 - l32 * g2
    c3 = g3 * d3
    c2 = g2 * d2 - l32 * c3
    c1 = g1 * d1 - l21 * c2 - l31 * c3
    return c1, c2, c3


def vmem(n):
    return [pl.BlockSpec(memory_space=pltpu.VMEM)] * n


def shape(*dims):
    return jax.ShapeDtypeStruct(dims, F32)


def call(kernel, inputs, outputs, scratch, mib, flops, in_specs=None, out_specs=None):
    many = isinstance(outputs, list)
    return pl.pallas_call(
        kernel,
        in_specs=in_specs or vmem(len(inputs)),
        out_specs=out_specs or (vmem(len(outputs)) if many else vmem(1)[0]),
        out_shape=outputs,
        scratch_shapes=scratch,
        compiler_params=pltpu.CompilerParams(vmem_limit_bytes=int(mib * 2**20)),
        cost_estimate=pl.CostEstimate(flops=flops, bytes_accessed=1 << 20, transcendentals=0),
    )(*inputs)


def per_device(previous, dissipated, material, coolant):
    given = (previous, dissipated, material, coolant)

    def buffer(dtype, *dims):
        return pltpu.VMEM(dims, dtype)

    edges = []
    for a in given:
        edges += [buffer(a.dtype, *a.shape[:-2], 8, TILE)] * 2
    a, b = call(
        pack_rows,
        [pltpu.with_memory_space_constraint(x, pltpu.HBM) for x in given],
        [pltpu.VMEM((FIELDS * HALO, TILE), F32)] * 2,
        edges + [pltpu.SemaphoreType.DMA((8,))],
        4,
        1 << 20,
        in_specs=[pl.BlockSpec(memory_space=pltpu.HBM)] * 4,
    )
    a, b = exchange(a, b, "gx")
    padded = TILE + 24
    c_blocks, q, y0, m0 = call(
        begin,
        given,
        [shape(4, TILE, TILE), shape(LAYERS, TILE + 8, TILE), shape(PAIRS, padded, TILE), shape(SCEN, 8, TILE)],
        [buffer(F32, LAYERS, padded, TILE), buffer(F32, PAIRS, padded, TILE)],
        8,
        1 << 27,
    )
    a, b, halo, c_halo = call(
        functools.partial(messages, lax.axis_size("gx")),
        (c_blocks, a, b),
        [shape(TILE + 8, TILE)] * 2 + [shape(FIELDS, 8, TILE), shape(4, 8, TILE)],
        [],
        4,
        1 << 20,
    )
    a, b = exchange(a, b, "gy")
    y1, y2, y0_fix, m = call(
        middle,
        (*given, halo, q, y0, m0),
        [shape(PAIRS, padded, TILE)] * 2 + [shape(PAIRS, 16, TILE), shape(SCEN * MOMENTS, 8, TILE)],
        [buffer(F32, LAYERS, 32, TILE)] + [buffer(F32, PAIRS, 32, TILE)] * 4,
        8,
        1 << 27,
    )
    devices = lax.axis_size("gx") * lax.axis_size("gy")
    ys, m = call(
        functools.partial(strips, lax.axis_size("gy")),
        (c_blocks, c_halo, a, b, m),
        [shape(3 * SCEN, TILE, TILE), shape(devices // 8, 8, TILE)],
        [buffer(F32, n, ROWS, TILE) for n in (2, 2, 4, 4, 4, 2, 4, 4, 4)],
        8,
        1 << 24,
    )
    everything = lax.all_to_all(m.reshape(devices, 1, TILE), ("gx", "gy"), split_axis=0, concat_axis=0, tiled=True)
    return call(
        combine,
        (previous, material, coolant, y0, y0_fix, y1, y2, ys, everything.reshape(devices // 8, 8, TILE)),
        shape(*previous.shape),
        [buffer(F32, *previous.shape), pltpu.SemaphoreType.DMA((4,))],
        8,
        1 << 24,
        out_specs=pl.BlockSpec(memory_space=pltpu.HBM),
    )


def solution(mesh):
    placed = (P(None, None, "gx", "gy"),) * 2 + (P(None, "gx", "gy"),) * 2
    return jax.shard_map(
        per_device, mesh=mesh, in_specs=placed, out_specs=P(None, None, "gx", "gy"), check_vma=False
    )
```

```python
import functools

import jax
import jax.numpy as jnp
from jax import lax
from jax.experimental import pallas as pl
from jax.experimental.pallas import tpu as pltpu
from jax.sharding import PartitionSpec as P

TIER_K = (1.0, 0.3, 0.12, 2.5)
CHANNEL_K = (1.0, 0.3, 0.25, 0.2)
CHANNEL_SINK = (0.0, 0.15, 0.45, 1.2)
TIER_HEAT = 0.05
CHANNEL_HEAT = 0.2
VERTICAL = 4.0

SCEN, TIERS, LAYERS = 2, 4, 7
PAIRS = SCEN * LAYERS
TILE = 128
HALO = 4
GROUP = 16
CHUNKS = TILE // 8
FIELDS = PAIRS + SCEN * TIERS + LAYERS
DISS = PAIRS
CODE = DISS + SCEN * TIERS
MOMENTS = 6
F32 = jnp.float32
ROOT, INVERSE, OVER, LOSS = range(4)


def tables(tier):
    if tier:
        kappa, sink, heat = TIER_K, (0.0,) * 4, TIER_HEAT
    else:
        kappa, sink, heat = CHANNEL_K, CHANNEL_SINK, CHANNEL_HEAT
    root = [k**0.5 for k in kappa]
    return (
        (0.0, *root),
        (0.0, *[1.0 / r for r in root]),
        (1.0, *[(heat + s) / r for s, r in zip(sink, root)]),
        (0.0, *[s / r for s, r in zip(sink, root)]),
    )


def pick(code, table):
    out = jnp.full(code.shape, table[0], F32)
    for index in range(1, 5):
        if table[index] != table[0]:
            out = jnp.where(code == float(index), F32(table[index]), out)
    return out


def pick_inside(code, table):
    out = jnp.full(code.shape, table[4], F32)
    for index in range(1, 4):
        if table[index] != table[4]:
            out = jnp.where(code == float(index), F32(table[index]), out)
    return out


def turn(x, shift, axis=1):
    shift %= x.shape[axis]
    return pltpu.roll(x, shift, axis) if shift else x


def tree(terms):
    while len(terms) > 1:
        terms = [terms[i] + terms[i + 1] if i + 1 < len(terms) else terms[i] for i in range(0, len(terms), 2)]
    return terms[0]


def field_rows(previous, dissipated, material, coolant, field, rows):
    if field < DISS:
        return previous[field // LAYERS, field % LAYERS, rows]
    if field < CODE:
        return dissipated[(field - DISS) // TIERS, (field - DISS) % TIERS, rows]
    layer = field - CODE
    block = material[layer // 2, rows] if layer % 2 == 0 else coolant[layer // 2, rows]
    return block.astype(F32) + 1.0


def pack_rows(prev, diss, mat, cool, b_out, a_out, pt, pb, dt, db, mt, mb, ct, cb, sems):
    copies = []
    for index, (source, top, bottom) in enumerate(((prev, pt, pb), (diss, dt, db), (mat, mt, mb), (cool, ct, cb))):
        lead = (slice(None),) * (len(source.shape) - 2)
        for side, (target, at) in enumerate(((top, 0), (bottom, TILE - 8))):
            copies.append(pltpu.make_async_copy(source.at[(*lead, pl.ds(at, 8))], target, sems.at[2 * index + side]))
    for copy in copies:
        copy.start()
    lower = lax.axis_index("gx") % 2 == 0
    for copy in copies:
        copy.wait()
    for field in range(FIELDS):
        top = field_rows(pt, dt, mt, ct, field, slice(0, HALO))
        bottom = field_rows(pb, db, mb, cb, field, slice(8 - HALO, 8))
        rows = slice(HALO * field, HALO * (field + 1))
        a_out[rows, :] = jnp.where(lower, bottom, top)
        b_out[rows, :] = jnp.where(lower, top, bottom)


def strips_of(get, lane):
    zero = jnp.zeros((8, TILE), F32)
    blocks = []
    for fields in (
        [(layer, layer) for layer in range(LAYERS)],
        [(layer, LAYERS + layer) for layer in range(LAYERS)],
        [(layer, CODE + layer) for layer in range(LAYERS)],
        [(2 * t + scen, DISS + TIERS * scen + t) for t in range(TIERS) for scen in range(SCEN)],
    ):
        out = zero
        for layer, field in fields:
            out = jnp.where(lane // GROUP == layer, turn(get(field), GROUP * layer + 8), out)
        blocks.append(out)
    return blocks


def neighbours(ref, base, r, x):
    out = []
    for layer in range(LAYERS):
        f = base + layer
        t = (ref[f, pl.ds(r - 1, 8), :] + ref[f, pl.ds(r + 1, 8), :]) + (turn(x[layer], 1) + turn(x[layer], -1))
        if layer == 0:
            t = t + VERTICAL * x[1]
        elif layer == LAYERS - 1:
            t = t + VERTICAL * x[layer - 1]
        else:
            t = t + VERTICAL * (x[layer - 1] + x[layer + 1])
        out.append(t)
    return out


def rows_of(ref, base, r, count=LAYERS):
    return [ref[base + i, pl.ds(r, 8), :] for i in range(count)]


def start_field(s, code, x, q, ss, syp, base, diss):
    ys, ts = [], []
    for layer in range(LAYERS):
        t = syp[layer] - (pick(code[layer], tables(False)[LOSS]) + ss[layer] if layer % 2 else ss[layer]) * x[layer]
        if layer % 2 == 0:
            t = t + diss[layer // 2] * pick(code[layer], tables(True)[INVERSE])
        ts.append(t)
        ys.append(q[layer] * t)
    return ys, ts


def begin(prev, diss, mat, cool, c_out, q_out, y0_out, m_out, s_ref, yp_ref):
    lane = lax.broadcasted_iota(jnp.int32, (8, TILE), 1)

    for k in range(CHUNKS):
        rows = slice(8 * k, 8 * k + 8)
        inner = slice(8 * k + 8, 8 * k + 16)
        x = [field_rows(prev, diss, mat, cool, f, rows) for f in range(FIELDS)]
        for index, block in enumerate(strips_of(lambda f: x[f], lane)):
            c_out[index, rows, :] = block
        for layer in range(LAYERS):
            s = pick_inside(x[CODE + layer], tables(layer % 2 == 0)[ROOT])
            s_ref[layer, inner, :] = s
            for scen in range(SCEN):
                yp_ref[scen * LAYERS + layer, inner, :] = s * x[scen * LAYERS + layer]

    acc = [jnp.zeros((8, TILE), F32)] * SCEN
    for k in range(CHUNKS):
        rows = slice(8 * k, 8 * k + 8)
        r = 8 * k + 8
        s = rows_of(s_ref, 0, r)
        code = [field_rows(prev, diss, mat, cool, CODE + layer, rows) for layer in range(LAYERS)]
        ss = neighbours(s_ref, 0, r, s)
        q = []
        for layer in range(LAYERS):
            q.append(s[layer] / (pick_inside(code[layer], tables(layer % 2 == 0)[OVER]) + ss[layer]))
            q_out[layer, rows, :] = q[layer]
        sums = []
        for scen in range(SCEN):
            base = scen * LAYERS
            syp = neighbours(yp_ref, base, r, rows_of(yp_ref, base, r))
            x = [prev[scen, layer, rows] for layer in range(LAYERS)]
            d = [diss[scen, t, rows] for t in range(TIERS)]
            y, t = start_field(s, code, x, q, ss, syp, base, d)
            for layer in range(LAYERS):
                y0_out[base + layer, pl.ds(r, 8), :] = y[layer]
            sums.append(tree([a * b for a, b in zip(y, t)]))
        if 0 < k < CHUNKS - 1:
            acc = [a + b for a, b in zip(acc, sums)]
    for scen in range(SCEN):
        m_out[scen] = acc[scen]


def messages(rows_of_devices, c_ref, b_in, a_in, b_out, a_out, halo_out, c_halo):
    lower = lax.axis_index("gx") % 2 == 0
    west = lax.axis_index("gy") % 2 == 0
    at_top, at_bottom = lax.axis_index("gx") == 0, lax.axis_index("gx") == rows_of_devices - 1
    lane = lax.broadcasted_iota(jnp.int32, (8, TILE), 1)
    for field in range(FIELDS):
        rows = slice(HALO * field, HALO * (field + 1))
        a, b = a_in[rows, :], b_in[rows, :]
        above, below = jnp.where(lower, b, a), jnp.where(lower, a, b)
        if field >= CODE:
            above = jnp.where(at_top, 0.0, above)
            below = jnp.where(at_bottom, 0.0, below)
        halo_out[field, :HALO, :] = above
        halo_out[field, HALO:, :] = below
    slot = lane % GROUP // HALO

    def send(blocks, rows):
        p0, p1, code, d = (turn(x, HALO * i - 8) for i, x in enumerate(blocks))

        def by_slot(a, b, c, e):
            return jnp.where(slot < 2, jnp.where(slot == 0, a, b), jnp.where(slot == 2, c, e))

        low, high = by_slot(p0, p1, code, d), by_slot(p1, code, d, p0)
        a_out[rows, :] = jnp.where(west, high, low)
        b_out[rows, :] = jnp.where(west, low, high)

    for k in range(CHUNKS):
        rows = slice(8 * k, 8 * k + 8)
        send([c_ref[i, rows, :] for i in range(4)], rows)
    blocks = strips_of(lambda f: halo_out[f], lane)
    for index in range(4):
        c_halo[index] = blocks[index]
    send(blocks, slice(TILE, TILE + 8))


def middle(prev, diss, mat, cool, halo, q_ref, y0, m_in, y1, y2, y0_fix, m_out, sn, ypn, y0n, y1n, y2n):
    zero = jnp.zeros((8, TILE), F32)

    def sweep(x_ref, out_ref):
        acc = [zero] * (SCEN if out_ref is None else 2 * SCEN)
        for k in range(CHUNKS):
            if out_ref is None and k in (0, CHUNKS - 1):
                continue
            rows = slice(8 * k, 8 * k + 8)
            r = 8 * k + 8
            odd, even = [], []
            for scen in range(SCEN):
                base = scen * LAYERS
                x = rows_of(x_ref, base, r)
                t = neighbours(x_ref, base, r, x)
                odd.append(tree([a * b for a, b in zip(x, t)]))
                if out_ref is not None:
                    p = []
                    for layer in range(LAYERS):
                        y = q_ref[layer, rows, :] * t[layer]
                        out_ref[base + layer, pl.ds(r, 8), :] = y
                        p.append(y * t[layer])
                    even.append(tree(p))
            if 0 < k < CHUNKS - 1:
                acc = [a + b for a, b in zip(acc, odd + even)]
        return acc

    m = [m_in[scen] for scen in range(SCEN)]
    m += sweep(y0, y1)
    m += sweep(y1, y2)
    m += sweep(y2, None)

    for side in range(2):
        own = 16 if side == 0 else 8
        beyond = 24 - own
        near = slice(0, 8) if side == 0 else slice(TILE - 8, TILE)
        inner = slice(8, 16) if side == 0 else slice(TILE - 16, TILE - 8)
        inner_at = 24 if side == 0 else 0
        chunks = (
            (own, lambda f: field_rows(prev, diss, mat, cool, f, near)),
            (inner_at, lambda f: field_rows(prev, diss, mat, cool, f, inner)),
            (beyond, lambda f: turn(halo[f], 4, 0)),
        )
        for at, get in chunks:
            for layer in range(LAYERS):
                s = pick(get(CODE + layer), tables(layer % 2 == 0)[ROOT])
                sn[layer, at : at + 8, :] = s
                for scen in range(SCEN):
                    ypn[scen * LAYERS + layer, at : at + 8, :] = s * get(scen * LAYERS + layer)
        padded_inner = slice(inner.start + 8, inner.stop + 8)
        padded_near = slice(near.start + 8, near.stop + 8)
        fix = slice(8 * side, 8 * side + 8)
        for f in range(PAIRS):
            y0n[f, inner_at : inner_at + 8, :] = y0[f, padded_inner, :]
            y1n[f, inner_at : inner_at + 8, :] = y1[f, padded_inner, :]
            y2n[f, inner_at : inner_at + 8, :] = y2[f, padded_inner, :]
        q = {}
        for at, get in (chunks[0], chunks[2]):
            s = rows_of(sn, 0, at)
            ss = neighbours(sn, 0, at, s)
            code = [get(CODE + layer) for layer in range(LAYERS)]
            q[at] = [s[i] / (pick(code[i], tables(i % 2 == 0)[OVER]) + ss[i]) for i in range(LAYERS)]
            for scen in range(SCEN):
                base = scen * LAYERS
                syp = neighbours(ypn, base, at, rows_of(ypn, base, at))
                x = [get(base + layer) for layer in range(LAYERS)]
                d = [get(DISS + scen * TIERS + t) for t in range(TIERS)]
                y, t = start_field(s, code, x, q[at], ss, syp, base, d)
                for layer in range(LAYERS):
                    y0n[base + layer, at : at + 8, :] = y[layer]
                    if at == own:
                        y0_fix[base + layer, fix, :] = y[layer]
                if at == own:
                    m[scen] = m[scen] + tree([a * b for a, b in zip(y, t)])
        for level, (x_ref, n_ref, out_ref) in enumerate(((y0n, y1n, y1), (y1n, y2n, y2), (y2n, None, None))):
            for at in (own, beyond) if n_ref is not None else (own,):
                for scen in range(SCEN):
                    base = scen * LAYERS
                    x = rows_of(x_ref, base, at)
                    t = neighbours(x_ref, base, at, x)
                    if at == own:
                        index = SCEN * (2 * level + 1) + scen
                        m[index] = m[index] + tree([a * b for a, b in zip(x, t)])
                    if n_ref is None:
                        continue
                    p = []
                    for layer in range(LAYERS):
                        y = q[at][layer] * t[layer]
                        n_ref[base + layer, at : at + 8, :] = y
                        if at == own:
                            out_ref[base + layer, padded_near, :] = y
                            p.append(y * t[layer])
                    if at == own:
                        index = SCEN * (2 * level + 2) + scen
                        m[index] = m[index] + tree(p)
    for index in range(SCEN * MOMENTS):
        m_out[index] = m[index]


TOP = 16
ROWS = TOP + TILE + 16


def strips(columns_of_devices, c_ref, c_halo, b_in, a_in, m_in, ys_out, m_out, code_ref, s_ref, x_ref, d_ref, yp_ref, q_ref, y0, y1, y2):
    west = lax.axis_index("gy") % 2 == 0
    lane = lax.broadcasted_iota(jnp.int32, (8, TILE), 1)
    outside = [lax.axis_index("gy") == end for end in (columns_of_devices - 1, 0)]
    place = lane % GROUP
    real = lane < GROUP * LAYERS
    tier = lane // GROUP % 2 == 0
    zero = jnp.zeros((8, TILE), F32)
    slot = place // HALO
    sides = (
        (place < 8, (place >= 8) & (place < 12), (place >= 4) & (place < 8) & real),
        (place >= 8, (place >= 4) & (place < 8), (place >= 8) & (place < 12) & real),
    )

    def lookup(code, kind):
        out = zero if tables(True)[kind][0] == 0.0 else jnp.full_like(zero, tables(True)[kind][0])
        for index in range(1, 5):
            value = jnp.where(tier, F32(tables(True)[kind][index]), F32(tables(False)[kind][index]))
            out = jnp.where(code == float(index), value, out)
        return out

    chunk_rows = [(slice(8 * k, 8 * k + 8), (8 * k + TOP,), 0) for k in range(CHUNKS)]
    chunk_rows.append((None, (TOP - 8, TOP + TILE), 4))
    for rows, targets, rotation in chunk_rows:
        message = slice(TILE, TILE + 8) if rows is None else rows
        a, b = a_in[message, :], b_in[message, :]
        blocks = [c_halo[i] if rows is None else c_ref[i, rows, :] for i in range(4)]
        east = jnp.where(outside[0], 0.0, jnp.where(west, a, b))
        wst = jnp.where(outside[1], 0.0, jnp.where(west, b, a))
        got = [turn(jnp.where(slot == i, east, wst), 8 - HALO * i) for i in range(4)]
        for side, (own, beyond, _) in enumerate(sides):
            full = [jnp.where(own, x, jnp.where(beyond, y, zero)) for x, y in zip(blocks, got)]
            full[2] = jnp.where(real, full[2], zero)
            full[3:] = [jnp.where(tier, full[3], zero), jnp.where(tier, turn(full[3], -GROUP), zero)]
            full = [turn(x, rotation, 0) for x in full]
            s = lookup(full[2], ROOT)
            for at in targets:
                here = slice(at, at + 8)
                code_ref[side, here, :] = full[2]
                s_ref[side, here, :] = s
                for scen in range(SCEN):
                    x_ref[2 * scen + side, here, :] = full[scen]
                    d_ref[2 * scen + side, here, :] = full[3 + scen]
                    yp_ref[2 * scen + side, here, :] = s * full[scen]

    def around(ref, index, at):
        x = ref[index, at : at + 8, :]
        lateral = (ref[index, at - 1 : at + 7, :] + ref[index, at + 1 : at + 9, :]) + (turn(x, 1) + turn(x, -1))
        return x, lateral + VERTICAL * (turn(x, GROUP) + turn(x, -GROUP))

    everywhere = range(TOP - 8, TOP + TILE + 8, 8)
    within = range(TOP, TOP + TILE, 8)
    m = [[zero, zero] for _ in range(SCEN * MOMENTS)]

    def count(index, side, at, value):
        if at in within:
            m[index][side] = m[index][side] + value

    for at in everywhere:
        here = slice(at, at + 8)
        for side in range(2):
            code = code_ref[side, here, :]
            s, ss = around(s_ref, side, at)
            q = s / (lookup(code, OVER) + ss)
            q_ref[side, here, :] = q
            inverse, loss = lookup(code, INVERSE), lookup(code, LOSS) + ss
            for scen in range(SCEN):
                f = 2 * scen + side
                _, syp = around(yp_ref, f, at)
                t = syp - loss * x_ref[f, here, :] + d_ref[f, here, :] * inverse
                y = q * t
                y0[f, here, :] = y
                count(scen, side, at, y * t)
    for level, (ref, out) in enumerate(((y0, y1), (y1, y2), (y2, None))):
        for at in everywhere if out is not None else within:
            here = slice(at, at + 8)
            for side in range(2):
                for scen in range(SCEN):
                    f = 2 * scen + side
                    x, t = around(ref, f, at)
                    count(SCEN * (2 * level + 1) + scen, side, at, x * t)
                    if out is not None:
                        y = q_ref[side, here, :] * t
                        out[f, here, :] = y
                        count(SCEN * (2 * level + 2) + scen, side, at, y * t)
    for level, ref in enumerate((y0, y1, y2)):
        for scen in range(SCEN):
            for k in range(CHUNKS):
                here = slice(8 * k + TOP, 8 * k + TOP + 8)
                merged = jnp.where(place < 8, ref[2 * scen, here, :], ref[2 * scen + 1, here, :])
                ys_out[SCEN * level + scen, 8 * k : 8 * k + 8, :] = merged
    line = lax.broadcasted_iota(jnp.int32, (8, TILE), 1)
    inner = (lane >= HALO) & (lane < TILE - HALO)
    out = zero
    for index in range(SCEN * MOMENTS):
        east, wst = (jnp.where(sides[side][2], m[index][side], 0.0) for side in range(2))
        value = jnp.where(inner, m_in[index], 0.0) + (east + wst)
        value = jnp.sum(jnp.sum(value, axis=0, keepdims=True), axis=1, keepdims=True)
        out = jnp.where(line == index, value, out)
    m_out[...] = jnp.broadcast_to(out, m_out.shape)


def combine(prev, mat, cool, y0, y0_fix, y1, y2, ys, m_ref, out, buffer, sems):
    lane = lax.broadcasted_iota(jnp.int32, (8, TILE), 1)
    edge = (lane < HALO) | (lane >= TILE - HALO)
    total = tree([m_ref[i] for i in range(m_ref.shape[0])])
    total = jnp.broadcast_to(jnp.sum(total, axis=0, keepdims=True), (8, TILE))
    weights = coefficients([turn(total, -SCEN * i) for i in range(MOMENTS)])
    c = [
        [jnp.broadcast_to(jnp.sum(jnp.where(lane == scen, w, 0.0), axis=1, keepdims=True), (8, TILE)) for w in weights]
        for scen in range(SCEN)
    ]
    parts = 4
    copies = []

    def chunk(k, at, first):
        rows = pl.ds(at, 8)
        padded = pl.ds(at + 8, 8)
        scale = [
            pick_inside(field_rows(prev, None, mat, cool, CODE + layer, rows), tables(layer % 2 == 0)[INVERSE])
            for layer in range(LAYERS)
        ]
        for scen in range(SCEN):
            strip = tree([c[scen][i] * ys[SCEN * i + scen, rows, :] for i in range(3)])
            for layer in range(LAYERS):
                f = scen * LAYERS + layer
                value = c[scen][1] * y1[f, padded, :] + c[scen][2] * y2[f, padded, :] + c[scen][0] * first(f)
                value = jnp.where(edge, turn(strip, 120 - GROUP * layer), value)
                buffer[scen, layer, rows, :] = prev[scen, layer, rows] + scale[layer] * value

    for part in range(parts):
        if part == 0:
            chunk(0, 0, lambda f: y0_fix[f, 0:8, :])
        low = max(1, part * CHUNKS // parts)
        high = min(CHUNKS - 1, (part + 1) * CHUNKS // parts)

        for k in range(low, high):
            chunk(k, 8 * k, lambda f, at=8 * k: y0[f, pl.ds(at + 8, 8), :])

        if part == parts - 1:
            chunk(CHUNKS - 1, TILE - 8, lambda f: y0_fix[f, 8:16, :])
        rows = pl.ds(part * TILE // parts, TILE // parts)
        copy = pltpu.make_async_copy(buffer.at[:, :, rows], out.at[:, :, rows], sems.at[part])
        copy.start()
        copies.append(copy)
    for copy in copies:
        copy.wait()


def swaps(devices):
    near = [(i, i ^ 1) for i in range(devices)]
    far = [(i, (i + 1) % devices) for i in range(1, devices, 2)]
    return near, far + [(b, a) for a, b in far]


def exchange(a, b, axis):
    near, far = swaps(lax.axis_size(axis))
    b = lax.ppermute(b, axis, far)
    return lax.ppermute(a, axis, near), b


def coefficients(m):
    h11, h12, h13, h23, h33 = (m[i] - m[i + 1] for i in range(5))
    h22 = h13

    def inverse(x):
        return jnp.where(x > 0, 1.0 / jnp.where(x > 0, x, 1.0), 0.0)

    d1 = inverse(h11)
    l21, l31 = h12 * d1, h13 * d1
    d2 = inverse(h22 - l21 * h12)
    u23 = h23 - l31 * h12
    l32 = u23 * d2
    d3 = inverse(h33 - l31 * h13 - l32 * u23)
    g1 = m[0]
    g2 = m[1] - l21 * g1
    g3 = m[2] - l31 * g1 - l32 * g2
    c3 = g3 * d3
    c2 = g2 * d2 - l32 * c3
    c1 = g1 * d1 - l21 * c2 - l31 * c3
    return c1, c2, c3


def vmem(n):
    return [pl.BlockSpec(memory_space=pltpu.VMEM)] * n


def shape(*dims):
    return jax.ShapeDtypeStruct(dims, F32)


def call(kernel, inputs, outputs, scratch, mib, flops, in_specs=None, out_specs=None):
    many = isinstance(outputs, list)
    return pl.pallas_call(
        kernel,
        in_specs=in_specs or vmem(len(inputs)),
        out_specs=out_specs or (vmem(len(outputs)) if many else vmem(1)[0]),
        out_shape=outputs,
        scratch_shapes=scratch,
        compiler_params=pltpu.CompilerParams(vmem_limit_bytes=int(mib * 2**20)),
        cost_estimate=pl.CostEstimate(flops=flops, bytes_accessed=1 << 20, transcendentals=0),
    )(*inputs)


def per_device(previous, dissipated, material, coolant):
    given = (previous, dissipated, material, coolant)

    def buffer(dtype, *dims):
        return pltpu.VMEM(dims, dtype)

    edges = []
    for a in given:
        edges += [buffer(a.dtype, *a.shape[:-2], 8, TILE)] * 2
    b, a = call(
        pack_rows,
        [pltpu.with_memory_space_constraint(x, pltpu.HBM) for x in given],
        [pltpu.VMEM((FIELDS * HALO, TILE), F32)] * 2,
        edges + [pltpu.SemaphoreType.DMA((8,))],
        4,
        1 << 20,
        in_specs=[pl.BlockSpec(memory_space=pltpu.HBM)] * 4,
    )
    a, b = exchange(a, b, "gx")
    padded = TILE + 24
    c_blocks, q, y0, m0 = call(
        begin,
        given,
        [shape(4, TILE, TILE), shape(LAYERS, TILE + 8, TILE), shape(PAIRS, padded, TILE), shape(SCEN, 8, TILE)],
        [buffer(F32, LAYERS, padded, TILE), buffer(F32, PAIRS, padded, TILE)],
        8,
        1 << 27,
    )
    b, a, halo, c_halo = call(
        functools.partial(messages, lax.axis_size("gx")),
        (c_blocks, b, a),
        [shape(TILE + 8, TILE)] * 2 + [shape(FIELDS, 8, TILE), shape(4, 8, TILE)],
        [],
        4,
        1 << 20,
    )
    a, b = exchange(a, b, "gy")
    y1, y2, y0_fix, m = call(
        middle,
        (*given, halo, q, y0, m0),
        [shape(PAIRS, padded, TILE)] * 2 + [shape(PAIRS, 16, TILE), shape(SCEN * MOMENTS, 8, TILE)],
        [buffer(F32, LAYERS, 32, TILE)] + [buffer(F32, PAIRS, 32, TILE)] * 4,
        8,
        1 << 27,
    )
    devices = lax.axis_size("gx") * lax.axis_size("gy")
    ys, m = call(
        functools.partial(strips, lax.axis_size("gy")),
        (c_blocks, c_halo, b, a, m),
        [shape(3 * SCEN, TILE, TILE), shape(devices // 8, 8, TILE)],
        [buffer(F32, n, ROWS, TILE) for n in (2, 2, 4, 4, 4, 2, 4, 4, 4)],
        8,
        1 << 24,
    )
    everything = lax.all_to_all(m.reshape(devices, 1, TILE), ("gx", "gy"), split_axis=0, concat_axis=0, tiled=True)
    return call(
        combine,
        (previous, material, coolant, y0, y0_fix, y1, y2, ys, everything.reshape(devices // 8, 8, TILE)),
        shape(*previous.shape),
        [buffer(F32, *previous.shape), pltpu.SemaphoreType.DMA((4,))],
        8,
        1 << 24,
        out_specs=pl.BlockSpec(memory_space=pltpu.HBM),
    )


def solution(mesh):
    placed = (P(None, None, "gx", "gy"),) * 2 + (P(None, "gx", "gy"),) * 2
    return jax.shard_map(
        per_device, mesh=mesh, in_specs=placed, out_specs=P(None, None, "gx", "gy"), check_vma=False
    )
```

```python
import functools

import jax
import jax.numpy as jnp
from jax import lax
from jax.experimental import pallas as pl
from jax.experimental.pallas import tpu as pltpu
from jax.sharding import PartitionSpec as P

TIER_K = (1.0, 0.3, 0.12, 2.5)
CHANNEL_K = (1.0, 0.3, 0.25, 0.2)
CHANNEL_SINK = (0.0, 0.15, 0.45, 1.2)
TIER_HEAT = 0.05
CHANNEL_HEAT = 0.2
VERTICAL = 4.0

SCEN, TIERS, LAYERS = 2, 4, 7
PAIRS = SCEN * LAYERS
TILE = 128
HALO = 4
GROUP = 16
CHUNKS = TILE // 8
FIELDS = PAIRS + SCEN * TIERS + LAYERS
DISS = PAIRS
CODE = DISS + SCEN * TIERS
MOMENTS = 6
F32 = jnp.float32
ROOT, INVERSE, OVER, LOSS = range(4)


def tables(tier):
    if tier:
        kappa, sink, heat = TIER_K, (0.0,) * 4, TIER_HEAT
    else:
        kappa, sink, heat = CHANNEL_K, CHANNEL_SINK, CHANNEL_HEAT
    root = [k**0.5 for k in kappa]
    return (
        (0.0, *root),
        (0.0, *[1.0 / r for r in root]),
        (1.0, *[(heat + s) / r for s, r in zip(sink, root)]),
        (0.0, *[s / r for s, r in zip(sink, root)]),
    )


def pick(code, table):
    out = jnp.full(code.shape, table[0], F32)
    for index in range(1, 5):
        if table[index] != table[0]:
            out = jnp.where(code == float(index), F32(table[index]), out)
    return out


def pick_inside(code, table):
    out = jnp.full(code.shape, table[4], F32)
    for index in range(1, 4):
        if table[index] != table[4]:
            out = jnp.where(code == float(index), F32(table[index]), out)
    return out


def turn(x, shift, axis=1):
    shift %= x.shape[axis]
    return pltpu.roll(x, shift, axis) if shift else x


def tree(terms):
    while len(terms) > 1:
        terms = [terms[i] + terms[i + 1] if i + 1 < len(terms) else terms[i] for i in range(0, len(terms), 2)]
    return terms[0]


def field_rows(previous, dissipated, material, coolant, field, rows):
    if field < DISS:
        return previous[field // LAYERS, field % LAYERS, rows]
    if field < CODE:
        return dissipated[(field - DISS) // TIERS, (field - DISS) % TIERS, rows]
    layer = field - CODE
    block = material[layer // 2, rows] if layer % 2 == 0 else coolant[layer // 2, rows]
    return block.astype(F32) + 1.0


def pack_rows(prev, diss, mat, cool, b_out, a_out, pt, pb, dt, db, mt, mb, ct, cb, sems):
    copies = []
    for index, (source, top, bottom) in enumerate(((prev, pt, pb), (diss, dt, db), (mat, mt, mb), (cool, ct, cb))):
        lead = (slice(None),) * (len(source.shape) - 2)
        for side, (target, at) in enumerate(((top, 0), (bottom, TILE - 8))):
            copies.append(pltpu.make_async_copy(source.at[(*lead, pl.ds(at, 8))], target, sems.at[2 * index + side]))
    for copy in copies:
        copy.start()
    lower = lax.axis_index("gx") % 2 == 0
    for copy in copies:
        copy.wait()
    for field in range(FIELDS):
        top = field_rows(pt, dt, mt, ct, field, slice(0, HALO))
        bottom = field_rows(pb, db, mb, cb, field, slice(8 - HALO, 8))
        rows = slice(HALO * field, HALO * (field + 1))
        a_out[rows, :] = jnp.where(lower, bottom, top)
        b_out[rows, :] = jnp.where(lower, top, bottom)


def strips_of(get, lane):
    zero = jnp.zeros((8, TILE), F32)
    blocks = []
    for fields in (
        [(layer, layer) for layer in range(LAYERS)],
        [(layer, LAYERS + layer) for layer in range(LAYERS)],
        [(layer, CODE + layer) for layer in range(LAYERS)],
        [(2 * t + scen, DISS + TIERS * scen + t) for t in range(TIERS) for scen in range(SCEN)],
    ):
        out = zero
        for layer, field in fields:
            out = jnp.where(lane // GROUP == layer, turn(get(field), GROUP * layer + 8), out)
        blocks.append(out)
    return blocks


def neighbours(ref, base, r, x):
    out = []
    for layer in range(LAYERS):
        f = base + layer
        t = (ref[f, pl.ds(r - 1, 8), :] + ref[f, pl.ds(r + 1, 8), :]) + (turn(x[layer], 1) + turn(x[layer], -1))
        if layer == 0:
            t = t + VERTICAL * x[1]
        elif layer == LAYERS - 1:
            t = t + VERTICAL * x[layer - 1]
        else:
            t = t + VERTICAL * (x[layer - 1] + x[layer + 1])
        out.append(t)
    return out


def rows_of(ref, base, r, count=LAYERS):
    return [ref[base + i, pl.ds(r, 8), :] for i in range(count)]


def start_field(s, code, x, q, ss, syp, base, diss):
    ys, ts = [], []
    for layer in range(LAYERS):
        t = syp[layer] - (pick(code[layer], tables(False)[LOSS]) + ss[layer] if layer % 2 else ss[layer]) * x[layer]
        if layer % 2 == 0:
            t = t + diss[layer // 2] * pick(code[layer], tables(True)[INVERSE])
        ts.append(t)
        ys.append(q[layer] * t)
    return ys, ts


def begin(prev, diss, mat, cool, c_out, q_out, y0_out, m_out, s_ref, yp_ref):
    lane = lax.broadcasted_iota(jnp.int32, (8, TILE), 1)

    for k in range(CHUNKS):
        rows = slice(8 * k, 8 * k + 8)
        inner = slice(8 * k + 8, 8 * k + 16)
        x = [field_rows(prev, diss, mat, cool, f, rows) for f in range(FIELDS)]
        for index, block in enumerate(strips_of(lambda f: x[f], lane)):
            c_out[index, rows, :] = block
        for layer in range(LAYERS):
            s = pick_inside(x[CODE + layer], tables(layer % 2 == 0)[ROOT])
            s_ref[layer, inner, :] = s
            for scen in range(SCEN):
                yp_ref[scen * LAYERS + layer, inner, :] = s * x[scen * LAYERS + layer]

    acc = [jnp.zeros((8, TILE), F32)] * SCEN
    for k in range(CHUNKS):
        rows = slice(8 * k, 8 * k + 8)
        r = 8 * k + 8
        s = rows_of(s_ref, 0, r)
        code = [field_rows(prev, diss, mat, cool, CODE + layer, rows) for layer in range(LAYERS)]
        ss = neighbours(s_ref, 0, r, s)
        q = []
        for layer in range(LAYERS):
            q.append(s[layer] / (pick_inside(code[layer], tables(layer % 2 == 0)[OVER]) + ss[layer]))
            q_out[layer, rows, :] = q[layer]
        sums = []
        for scen in range(SCEN):
            base = scen * LAYERS
            syp = neighbours(yp_ref, base, r, rows_of(yp_ref, base, r))
            x = [prev[scen, layer, rows] for layer in range(LAYERS)]
            d = [diss[scen, t, rows] for t in range(TIERS)]
            y, t = start_field(s, code, x, q, ss, syp, base, d)
            for layer in range(LAYERS):
                y0_out[base + layer, pl.ds(r, 8), :] = y[layer]
            sums.append(tree([a * b for a, b in zip(y, t)]))
        if 0 < k < CHUNKS - 1:
            acc = [a + b for a, b in zip(acc, sums)]
    for scen in range(SCEN):
        m_out[scen] = acc[scen]


def messages(rows_of_devices, c_ref, b_in, a_in, b_out, a_out, halo_out, c_halo):
    lower = lax.axis_index("gx") % 2 == 0
    west = lax.axis_index("gy") % 2 == 0
    at_top, at_bottom = lax.axis_index("gx") == 0, lax.axis_index("gx") == rows_of_devices - 1
    lane = lax.broadcasted_iota(jnp.int32, (8, TILE), 1)
    for field in range(FIELDS):
        rows = slice(HALO * field, HALO * (field + 1))
        a, b = a_in[rows, :], b_in[rows, :]
        above, below = jnp.where(lower, b, a), jnp.where(lower, a, b)
        if field >= CODE:
            above = jnp.where(at_top, 0.0, above)
            below = jnp.where(at_bottom, 0.0, below)
        halo_out[field, :HALO, :] = above
        halo_out[field, HALO:, :] = below
    slot = lane % GROUP // HALO

    def send(blocks, rows):
        p0, p1, code, d = (turn(x, HALO * i - 8) for i, x in enumerate(blocks))

        def by_slot(a, b, c, e):
            return jnp.where(slot < 2, jnp.where(slot == 0, a, b), jnp.where(slot == 2, c, e))

        low, high = by_slot(p0, p1, code, d), by_slot(p1, code, d, p0)
        a_out[rows, :] = jnp.where(west, high, low)
        b_out[rows, :] = jnp.where(west, low, high)

    for k in range(CHUNKS):
        rows = slice(8 * k, 8 * k + 8)
        send([c_ref[i, rows, :] for i in range(4)], rows)
    blocks = strips_of(lambda f: halo_out[f], lane)
    for index in range(4):
        c_halo[index] = blocks[index]
    send(blocks, slice(TILE, TILE + 8))


def middle(prev, diss, mat, cool, halo, q_ref, y0, m_in, y1, y2, y0_fix, m_out, sn, ypn, y0n, y1n, y2n):
    zero = jnp.zeros((8, TILE), F32)

    def sweep(x_ref, out_ref):
        acc = [zero] * (SCEN if out_ref is None else 2 * SCEN)
        for k in range(CHUNKS):
            if out_ref is None and k in (0, CHUNKS - 1):
                continue
            rows = slice(8 * k, 8 * k + 8)
            r = 8 * k + 8
            odd, even = [], []
            for scen in range(SCEN):
                base = scen * LAYERS
                x = rows_of(x_ref, base, r)
                t = neighbours(x_ref, base, r, x)
                odd.append(tree([a * b for a, b in zip(x, t)]))
                if out_ref is not None:
                    p = []
                    for layer in range(LAYERS):
                        y = q_ref[layer, rows, :] * t[layer]
                        out_ref[base + layer, pl.ds(r, 8), :] = y
                        p.append(y * t[layer])
                    even.append(tree(p))
            if 0 < k < CHUNKS - 1:
                acc = [a + b for a, b in zip(acc, odd + even)]
        return acc

    m = [m_in[scen] for scen in range(SCEN)]
    m += sweep(y0, y1)
    m += sweep(y1, y2)
    m += sweep(y2, None)

    for side in range(2):
        own = 16 if side == 0 else 8
        beyond = 24 - own
        near = slice(0, 8) if side == 0 else slice(TILE - 8, TILE)
        inner = slice(8, 16) if side == 0 else slice(TILE - 16, TILE - 8)
        inner_at = 24 if side == 0 else 0
        chunks = (
            (own, lambda f: field_rows(prev, diss, mat, cool, f, near)),
            (inner_at, lambda f: field_rows(prev, diss, mat, cool, f, inner)),
            (beyond, lambda f: turn(halo[f], 4, 0)),
        )
        for at, get in chunks:
            for layer in range(LAYERS):
                s = pick(get(CODE + layer), tables(layer % 2 == 0)[ROOT])
                sn[layer, at : at + 8, :] = s
                for scen in range(SCEN):
                    ypn[scen * LAYERS + layer, at : at + 8, :] = s * get(scen * LAYERS + layer)
        padded_inner = slice(inner.start + 8, inner.stop + 8)
        padded_near = slice(near.start + 8, near.stop + 8)
        fix = slice(8 * side, 8 * side + 8)
        for f in range(PAIRS):
            y0n[f, inner_at : inner_at + 8, :] = y0[f, padded_inner, :]
            y1n[f, inner_at : inner_at + 8, :] = y1[f, padded_inner, :]
            y2n[f, inner_at : inner_at + 8, :] = y2[f, padded_inner, :]
        q = {}
        for at, get in (chunks[0], chunks[2]):
            s = rows_of(sn, 0, at)
            ss = neighbours(sn, 0, at, s)
            code = [get(CODE + layer) for layer in range(LAYERS)]
            q[at] = [s[i] / (pick(code[i], tables(i % 2 == 0)[OVER]) + ss[i]) for i in range(LAYERS)]
            for scen in range(SCEN):
                base = scen * LAYERS
                syp = neighbours(ypn, base, at, rows_of(ypn, base, at))
                x = [get(base + layer) for layer in range(LAYERS)]
                d = [get(DISS + scen * TIERS + t) for t in range(TIERS)]
                y, t = start_field(s, code, x, q[at], ss, syp, base, d)
                for layer in range(LAYERS):
                    y0n[base + layer, at : at + 8, :] = y[layer]
                    if at == own:
                        y0_fix[base + layer, fix, :] = y[layer]
                if at == own:
                    m[scen] = m[scen] + tree([a * b for a, b in zip(y, t)])
        for level, (x_ref, n_ref, out_ref) in enumerate(((y0n, y1n, y1), (y1n, y2n, y2), (y2n, None, None))):
            for at in (own, beyond) if n_ref is not None else (own,):
                for scen in range(SCEN):
                    base = scen * LAYERS
                    x = rows_of(x_ref, base, at)
                    t = neighbours(x_ref, base, at, x)
                    if at == own:
                        index = SCEN * (2 * level + 1) + scen
                        m[index] = m[index] + tree([a * b for a, b in zip(x, t)])
                    if n_ref is None:
                        continue
                    p = []
                    for layer in range(LAYERS):
                        y = q[at][layer] * t[layer]
                        n_ref[base + layer, at : at + 8, :] = y
                        if at == own:
                            out_ref[base + layer, padded_near, :] = y
                            p.append(y * t[layer])
                    if at == own:
                        index = SCEN * (2 * level + 2) + scen
                        m[index] = m[index] + tree(p)
    for index in range(SCEN * MOMENTS):
        m_out[index] = m[index]


TOP = 16
ROWS = TOP + TILE + 24


def strips(columns_of_devices, c_ref, c_halo, b_in, a_in, m_in, ys_out, m_out, code_ref, s_ref, x_ref, d_ref, yp_ref, q_ref, y0, y1, y2):
    west = lax.axis_index("gy") % 2 == 0
    lane = lax.broadcasted_iota(jnp.int32, (8, TILE), 1)
    outside = [lax.axis_index("gy") == end for end in (columns_of_devices - 1, 0)]
    place = lane % GROUP
    real = lane < GROUP * LAYERS
    tier = lane // GROUP % 2 == 0
    zero = jnp.zeros((8, TILE), F32)
    slot = place // HALO
    sides = (
        (place < 8, (place >= 8) & (place < 12), (place >= 4) & (place < 8) & real),
        (place >= 8, (place >= 4) & (place < 8), (place >= 8) & (place < 12) & real),
    )

    def lookup(code, kind):
        out = zero if tables(True)[kind][0] == 0.0 else jnp.full_like(zero, tables(True)[kind][0])
        for index in range(1, 5):
            value = jnp.where(tier, F32(tables(True)[kind][index]), F32(tables(False)[kind][index]))
            out = jnp.where(code == float(index), value, out)
        return out

    chunk_rows = [(slice(8 * k, 8 * k + 8), (8 * k + TOP,), 0) for k in range(CHUNKS)]
    chunk_rows.append((None, (TOP - 8, TOP + TILE), 4))
    for rows, targets, rotation in chunk_rows:
        message = slice(TILE, TILE + 8) if rows is None else rows
        a, b = a_in[message, :], b_in[message, :]
        blocks = [c_halo[i] if rows is None else c_ref[i, rows, :] for i in range(4)]
        east = jnp.where(outside[0], 0.0, jnp.where(west, a, b))
        wst = jnp.where(outside[1], 0.0, jnp.where(west, b, a))
        got = [turn(jnp.where(slot == i, east, wst), 8 - HALO * i) for i in range(4)]
        for side, (own, beyond, _) in enumerate(sides):
            full = [jnp.where(own, x, jnp.where(beyond, y, zero)) for x, y in zip(blocks, got)]
            full[2] = jnp.where(real, full[2], zero)
            full[3:] = [jnp.where(tier, full[3], zero), jnp.where(tier, turn(full[3], -GROUP), zero)]
            full = [turn(x, rotation, 0) for x in full]
            s = lookup(full[2], ROOT)
            for at in targets:
                here = slice(at, at + 8)
                code_ref[side, here, :] = full[2]
                s_ref[side, here, :] = s
                for scen in range(SCEN):
                    x_ref[2 * scen + side, here, :] = full[scen]
                    d_ref[2 * scen + side, here, :] = full[3 + scen]
                    yp_ref[2 * scen + side, here, :] = s * full[scen]

    def around(ref, index, at):
        x = ref[index, at : at + 8, :]
        lateral = (ref[index, at - 1 : at + 7, :] + ref[index, at + 1 : at + 9, :]) + (turn(x, 1) + turn(x, -1))
        return x, lateral + VERTICAL * (turn(x, GROUP) + turn(x, -GROUP))

    everywhere = range(TOP - 8, TOP + TILE + 8, 8)
    within = range(TOP, TOP + TILE, 8)
    m = [[zero, zero] for _ in range(SCEN * MOMENTS)]

    def count(index, side, at, value):
        if at in within:
            m[index][side] = m[index][side] + value

    for at in everywhere:
        here = slice(at, at + 8)
        for side in range(2):
            code = code_ref[side, here, :]
            s, ss = around(s_ref, side, at)
            q = s / (lookup(code, OVER) + ss)
            q_ref[side, here, :] = q
            inverse, loss = lookup(code, INVERSE), lookup(code, LOSS) + ss
            for scen in range(SCEN):
                f = 2 * scen + side
                _, syp = around(yp_ref, f, at)
                t = syp - loss * x_ref[f, here, :] + d_ref[f, here, :] * inverse
                y = q * t
                y0[f, here, :] = y
                count(scen, side, at, y * t)
    for level, (ref, out) in enumerate(((y0, y1), (y1, y2), (y2, None))):
        for at in everywhere if out is not None else within:
            here = slice(at, at + 8)
            for side in range(2):
                for scen in range(SCEN):
                    f = 2 * scen + side
                    x, t = around(ref, f, at)
                    count(SCEN * (2 * level + 1) + scen, side, at, x * t)
                    if out is not None:
                        y = q_ref[side, here, :] * t
                        out[f, here, :] = y
                        count(SCEN * (2 * level + 2) + scen, side, at, y * t)
    for level, ref in enumerate((y0, y1, y2)):
        for scen in range(SCEN):
            for k in range(CHUNKS):
                here = slice(8 * k + TOP, 8 * k + TOP + 8)
                merged = jnp.where(place < 8, ref[2 * scen, here, :], ref[2 * scen + 1, here, :])
                ys_out[SCEN * level + scen, 8 * k : 8 * k + 8, :] = merged
    line = lax.broadcasted_iota(jnp.int32, (8, TILE), 1)
    inner = (lane >= HALO) & (lane < TILE - HALO)
    out = zero
    for index in range(SCEN * MOMENTS):
        east, wst = (jnp.where(sides[side][2], m[index][side], 0.0) for side in range(2))
        value = jnp.where(inner, m_in[index], 0.0) + (east + wst)
        value = jnp.sum(jnp.sum(value, axis=0, keepdims=True), axis=1, keepdims=True)
        out = jnp.where(line == index, value, out)
    m_out[...] = jnp.broadcast_to(out, m_out.shape)


def combine(prev, mat, cool, y0, y0_fix, y1, y2, ys, m_ref, out, buffer, sems):
    lane = lax.broadcasted_iota(jnp.int32, (8, TILE), 1)
    edge = (lane < HALO) | (lane >= TILE - HALO)
    total = tree([m_ref[i] for i in range(m_ref.shape[0])])
    total = jnp.broadcast_to(jnp.sum(total, axis=0, keepdims=True), (8, TILE))
    weights = coefficients([turn(total, -SCEN * i) for i in range(MOMENTS)])
    c = [
        [jnp.broadcast_to(jnp.sum(jnp.where(lane == scen, w, 0.0), axis=1, keepdims=True), (8, TILE)) for w in weights]
        for scen in range(SCEN)
    ]
    parts = 8
    copies = []

    def chunk(k, at, first):
        rows = pl.ds(at, 8)
        padded = pl.ds(at + 8, 8)
        scale = [
            pick_inside(field_rows(prev, None, mat, cool, CODE + layer, rows), tables(layer % 2 == 0)[INVERSE])
            for layer in range(LAYERS)
        ]
        for scen in range(SCEN):
            strip = tree([c[scen][i] * ys[SCEN * i + scen, rows, :] for i in range(3)])
            for layer in range(LAYERS):
                f = scen * LAYERS + layer
                value = c[scen][1] * y1[f, padded, :] + c[scen][2] * y2[f, padded, :] + c[scen][0] * first(f)
                value = jnp.where(edge, turn(strip, 120 - GROUP * layer), value)
                buffer[scen, layer, rows, :] = prev[scen, layer, rows] + scale[layer] * value

    for part in range(parts):
        if part == 0:
            chunk(0, 0, lambda f: y0_fix[f, 0:8, :])
        low = max(1, part * CHUNKS // parts)
        high = min(CHUNKS - 1, (part + 1) * CHUNKS // parts)

        for k in range(low, high):
            chunk(k, 8 * k, lambda f, at=8 * k: y0[f, pl.ds(at + 8, 8), :])

        if part == parts - 1:
            chunk(CHUNKS - 1, TILE - 8, lambda f: y0_fix[f, 8:16, :])
        rows = pl.ds(part * TILE // parts, TILE // parts)
        copy = pltpu.make_async_copy(buffer.at[:, :, rows], out.at[:, :, rows], sems.at[part])
        copy.start()
        copies.append(copy)
    for copy in copies:
        copy.wait()


def swaps(devices):
    near = [(i, i ^ 1) for i in range(devices)]
    far = [(i, (i + 1) % devices) for i in range(1, devices, 2)]
    return near, far + [(b, a) for a, b in far]


def exchange(a, b, axis):
    near, far = swaps(lax.axis_size(axis))
    b = lax.ppermute(b, axis, far)
    return lax.ppermute(a, axis, near), b


def coefficients(m):
    h11, h12, h13, h23, h33 = (m[i] - m[i + 1] for i in range(5))
    h22 = h13

    def inverse(x):
        return jnp.where(x > 0, 1.0 / jnp.where(x > 0, x, 1.0), 0.0)

    d1 = inverse(h11)
    l21, l31 = h12 * d1, h13 * d1
    d2 = inverse(h22 - l21 * h12)
    u23 = h23 - l31 * h12
    l32 = u23 * d2
    d3 = inverse(h33 - l31 * h13 - l32 * u23)
    g1 = m[0]
    g2 = m[1] - l21 * g1
    g3 = m[2] - l31 * g1 - l32 * g2
    c3 = g3 * d3
    c2 = g2 * d2 - l32 * c3
    c1 = g1 * d1 - l21 * c2 - l31 * c3
    return c1, c2, c3


def vmem(n):
    return [pl.BlockSpec(memory_space=pltpu.VMEM)] * n


def shape(*dims):
    return jax.ShapeDtypeStruct(dims, F32)


def call(kernel, inputs, outputs, scratch, mib, flops, in_specs=None, out_specs=None):
    many = isinstance(outputs, list)
    return pl.pallas_call(
        kernel,
        in_specs=in_specs or vmem(len(inputs)),
        out_specs=out_specs or (vmem(len(outputs)) if many else vmem(1)[0]),
        out_shape=outputs,
        scratch_shapes=scratch,
        compiler_params=pltpu.CompilerParams(vmem_limit_bytes=int(mib * 2**20)),
        cost_estimate=pl.CostEstimate(flops=flops, bytes_accessed=1 << 20, transcendentals=0),
    )(*inputs)


def per_device(previous, dissipated, material, coolant):
    given = (previous, dissipated, material, coolant)

    def buffer(dtype, *dims):
        return pltpu.VMEM(dims, dtype)

    edges = []
    for a in given:
        edges += [buffer(a.dtype, *a.shape[:-2], 8, TILE)] * 2
    b, a = call(
        pack_rows,
        [pltpu.with_memory_space_constraint(x, pltpu.HBM) for x in given],
        [pltpu.VMEM((FIELDS * HALO, TILE), F32)] * 2,
        edges + [pltpu.SemaphoreType.DMA((8,))],
        4,
        1 << 20,
        in_specs=[pl.BlockSpec(memory_space=pltpu.HBM)] * 4,
    )
    a, b = exchange(a, b, "gx")
    padded = TILE + 24
    c_blocks, q, y0, m0 = call(
        begin,
        given,
        [shape(4, TILE, TILE), shape(LAYERS, TILE + 8, TILE), shape(PAIRS, padded, TILE), shape(SCEN, 8, TILE)],
        [buffer(F32, LAYERS, padded, TILE), buffer(F32, PAIRS, padded, TILE)],
        8,
        1 << 27,
    )
    b, a, halo, c_halo = call(
        functools.partial(messages, lax.axis_size("gx")),
        (c_blocks, b, a),
        [shape(TILE + 8, TILE)] * 2 + [shape(FIELDS, 8, TILE), shape(4, 8, TILE)],
        [],
        4,
        1 << 20,
    )
    a, b = exchange(a, b, "gy")
    y1, y2, y0_fix, m = call(
        middle,
        (*given, halo, q, y0, m0),
        [shape(PAIRS, padded, TILE)] * 2 + [shape(PAIRS, 16, TILE), shape(SCEN * MOMENTS, 8, TILE)],
        [buffer(F32, LAYERS, 32, TILE)] + [buffer(F32, PAIRS, 32, TILE)] * 4,
        8,
        1 << 27,
    )
    devices = lax.axis_size("gx") * lax.axis_size("gy")
    ys, m = call(
        functools.partial(strips, lax.axis_size("gy")),
        (c_blocks, c_halo, b, a, m),
        [shape(3 * SCEN, TILE, TILE), shape(devices // 8, 8, TILE)],
        [buffer(F32, n, ROWS, TILE) for n in (2, 2, 4, 4, 4, 2, 4, 4, 4)],
        8,
        1 << 24,
    )
    everything = lax.all_to_all(m.reshape(devices, 1, TILE), ("gx", "gy"), split_axis=0, concat_axis=0, tiled=True)
    return call(
        combine,
        (previous, material, coolant, y0, y0_fix, y1, y2, ys, everything.reshape(devices // 8, 8, TILE)),
        shape(*previous.shape),
        [buffer(F32, *previous.shape), pltpu.SemaphoreType.DMA((8,))],
        8,
        1 << 24,
        out_specs=pl.BlockSpec(memory_space=pltpu.HBM),
    )


def solution(mesh):
    placed = (P(None, None, "gx", "gy"),) * 2 + (P(None, "gx", "gy"),) * 2
    return jax.shard_map(
        per_device, mesh=mesh, in_specs=placed, out_specs=P(None, None, "gx", "gy"), check_vma=False
    )
```
